128 devices in a mesh: gx: 4 (over x_lo, core), gy: 4 (over y), gz: 8 (over z, x_hi).
Axes of the slice: x: 4 (x_hi: 2, x_lo: 2; x = x_hi * 2 + x_lo), y: 4, z: 4, core: 2. Of those that a mesh axis runs over, the one named last changes fastest.
Arguments:
- orbitals: float32 [64, 32, 32, 1024], P(None, 'gx', 'gy', 'gz'), may hold values from -6 to 6
- potential: float32 [32, 32, 1024], P('gx', 'gy', 'gz'), may hold values from 0 to 0.5
- centre: float32 [64], replicated, may hold values from 3 to 5
- half_width: float32 [64], replicated, may hold values from 3 to 5
Outputs:
- filtered: float32 [64, 32, 32, 1024], P(None, 'gx', 'gy', 'gz')
The draws below stay inside these ranges and needn't reach their ends.
All inputs are finite; a program needn't handle non-finite values.
Results may differ from the reference program's by a relative error of at most 0.00002.
Values sent between devices are 32-bit elements; how exact they have to be, the bound alone decides.
No kernel may reach another device: no remote copies, remote signals or barrier semaphores. Data moves between devices by JAX's collectives and lax.ppermute only.
A program may use at most 64 MiB of HBM per device.

```python
import jax
import jax.numpy as jnp
from jax import lax

BANDS = 64
NX = 32
NY = 32
NZ = 1024


def block_levels(rng, shape, split, least, top_value):
    def one(axis_at, blocks):
        heights = jax.random.uniform(jax.random.fold_in(jax.random.fold_in(rng, 6), axis_at), (blocks,), jnp.float32, least / len(split), top_value / len(split))
        return jnp.repeat(jnp.exp(heights), shape[axis_at] // blocks).reshape((-1,) + (1,) * (len(shape) - axis_at - 1))

    level = one(*split[0])
    for cut in split[1:]:
        level = level * one(*cut)
    return level


def gaussian(stream_key, dims, scale, bound, split=(), dtype=jnp.bfloat16):
    result = jax.random.normal(stream_key, dims, jnp.float32) * scale
    if len(split) > 0:
        result = block_levels(stream_key, dims, split, -0.22, 0.18) * result
    return jnp.clip(result, min=-bound, max=bound).astype(dtype)


def setup_inputs(seed: int = 0) -> dict:
    key_of = jax.random.split(jax.random.key(seed), 5)
    orbitals = gaussian(key_of[0], (BANDS, NX, NY, NZ), 1.0, 6.0, ((1, 4), (2, 4), (3, 8)), jnp.float32)
    potential = jnp.clip(0.5 * jax.random.uniform(key_of[1], (NX, NY, NZ), jnp.float32) ** block_levels(key_of[1], (NX, NY, NZ), ((0, 4), (1, 4), (2, 8)), -0.2, 0.2), 0.0, 0.5)
    centre = jnp.clip(jax.random.uniform(key_of[2], (BANDS,), jnp.float32, 3.0, 5.0), 3.0, 5.0)
    half_width = jnp.clip(jax.random.uniform(key_of[3], (BANDS,), jnp.float32, 3.0, 5.0), 3.0, 5.0)
    return {"orbitals": orbitals, "potential": potential, "centre": centre, "half_width": half_width}


shift_mass = 0.05
jacobi_weight = 2.0 / 3.0


def neighbour_sum(field):
    total = jnp.roll(field, 1, 0) + jnp.roll(field, -1, 0)
    total = total + jnp.roll(field, 1, 1) + jnp.roll(field, -1, 1)
    return total + jnp.roll(field, 1, 2) + jnp.roll(field, -1, 2)


def operate(field, diagonal, coupling):
    return diagonal * field - coupling * neighbour_sum(field)


def restrict(field):
    shape = field.shape
    return 0.5 * field.reshape(shape[0] // 2, 2, shape[1] // 2, 2, shape[2] // 2, 2).sum(axis=(1, 3, 5))


def average_cells(field):
    shape = field.shape
    return 0.125 * field.reshape(shape[0] // 2, 2, shape[1] // 2, 2, shape[2] // 2, 2).sum(axis=(1, 3, 5))


def prolong(field):
    return jnp.repeat(jnp.repeat(jnp.repeat(field, 2, 0), 2, 1), 2, 2)


def relax(level, source, diagonal, coupling):
    return level + jacobi_weight * (source - operate(level, diagonal, coupling)) / diagonal


def reference(orbitals, potential, centre, half_width):
    potential_one = average_cells(potential)
    potential_two = average_cells(potential_one)
    diagonal_fine = 3.0 + potential
    diagonal_one = 0.75 + potential_one + shift_mass
    diagonal_two = 0.1875 + potential_two + shift_mass

    def one_band(packed):
        orbital, middle, spread = packed
        first_image = operate(orbital, diagonal_fine, 0.5)
        first_order = (first_image - middle * orbital) / spread
        second_image = operate(first_order, diagonal_fine, 0.5)
        second_order = 2.0 * (second_image - middle * first_order) / spread - orbital
        source_one = restrict(second_order)
        level_one = jacobi_weight * source_one / diagonal_one
        level_one = relax(level_one, source_one, diagonal_one, 0.125)
        residue = source_one - operate(level_one, diagonal_one, 0.125)
        source_two = restrict(residue)
        level_two = jacobi_weight * source_two / diagonal_two
        for sweep_index in range(2):
            level_two = relax(level_two, source_two, diagonal_two, 0.03125)
        level_one = level_one + prolong(level_two)
        level_one = relax(level_one, source_one, diagonal_one, 0.125)
        return second_order + prolong(level_one)

    return lax.map(one_band, (orbitals, centre, half_width))
```

```python
import functools

import jax
import jax.numpy as jnp
from jax import lax
from jax.experimental import pallas as pl
from jax.experimental.pallas import tpu as pltpu
from jax.sharding import PartitionSpec as P

BANDS = 64
TILE = (8, 128)
GROUPS = 16
weight = 2.0 / 3.0

VMEM = pl.BlockSpec(memory_space=pltpu.VMEM)
SMEM = pl.BlockSpec(memory_space=pltpu.SMEM)


def shape(*dims):
    return jax.ShapeDtypeStruct(dims, jnp.float32)


def call(body, ins, outs, scratch=(), aliases=None, flops=4_000_000):
    return pl.pallas_call(
        body,
        out_shape=outs,
        in_specs=ins,
        out_specs=tuple(VMEM for _ in outs),
        scratch_shapes=scratch,
        input_output_aliases=aliases or {},
        compiler_params=pltpu.CompilerParams(vmem_limit_bytes=16 * 1024 * 1024),
        cost_estimate=pl.CostEstimate(flops=flops, bytes_accessed=4_000_000, transcendentals=0),
    )


def lanes():
    return lax.broadcasted_iota(jnp.int32, TILE, 1)


def rows():
    return lax.broadcasted_iota(jnp.int32, TILE, 0)


def lroll(v, shift):
    return pltpu.roll(v, shift, 1)


def sroll(v, shift):
    return pltpu.roll(v, shift, 0)


def plane(x):
    return pl.ds(x * 8, 8)


def nearest(lane, zp, zm, x):
    return jnp.where((lane & 1) == 0, zp[x], zm[x])


def pack_fine(orb, pot, xhi, xlo, yhi, ylo, zhi, zlo):
    lane = lanes()

    def put(carry, v, slot):
        high, low = carry
        turned = lroll(v, (2 * slot + 2) & 127)
        high = jnp.where((lane >> 1) == slot, turned, high)
        low = jnp.where((lane >> 1) == ((slot + 1) & 63), turned, low)
        return high, low

    def body(b, carry):
        done = []
        for x in range(8):
            v = orb[b, plane(x), :]
            done.append(put(carry[x], v, b))
            if x == 7:
                xhi[b] = v
            if x == 0:
                xlo[b] = v
        yhi[b] = orb[b, pl.ds(7, 8, stride=8), :]
        ylo[b] = orb[b, pl.ds(0, 8, stride=8), :]
        return tuple(done)

    zero = jnp.zeros(TILE, jnp.float32)
    carry = lax.fori_loop(0, BANDS, body, tuple((zero, zero) for _ in range(8)))
    for x in range(8):
        zhi[x] = carry[x][0]
        zlo[x] = lroll(carry[x][1], 126)
    edge = (zero, zero)
    for x in range(8):
        edge = put(edge, pot[plane(x), :], x)
    zhi[8] = edge[0]
    zlo[8] = lroll(edge[1], 126)


def star(v, x, b, get, xm, xp, ym, yp, halo, lane, row):
    left = get(x - 1) if x > 0 else xm[b]
    right = get(x + 1) if x < 7 else xp[b]
    h = lroll(halo, 127 - 2 * b)
    total = left + right
    up = jnp.where(row == 7, yp[b, pl.ds(x, 1), :], sroll(v, 7))
    down = jnp.where(row == 0, ym[b, pl.ds(x, 1), :], sroll(v, 1))
    total = total + (up + down)
    ahead = jnp.where(lane == 127, h, lroll(v, 127))
    behind = jnp.where(lane == 0, h, lroll(v, 1))
    return total + (ahead + behind)


def first_image(
    middle, inverse, orb, pot, xm, xp, ym, yp, zm, zp, first, xhi, xlo, yhi, ylo, near
):
    lane, row = lanes(), rows()
    for x in range(8):
        near[plane(x), :] = nearest(lane, zp, zm, x)

    def body(b, _):
        c, r = middle[b], inverse[b]
        get = lambda x: orb[b, plane(x), :]
        for x in range(8):
            v = get(x)
            total = star(v, x, b, get, xm, xp, ym, yp, near[plane(x), :], lane, row)
            value = (((3.0 - c) + pot[plane(x), :]) * v - 0.5 * total) * r
            first[b, plane(x), :] = value
            if x == 7:
                xhi[b] = value
            if x == 0:
                xlo[b] = value
        yhi[b] = first[b, pl.ds(7, 8, stride=8), :]
        ylo[b] = first[b, pl.ds(0, 8, stride=8), :]
        return 0

    lax.fori_loop(0, BANDS, body, 0)
    xhi[BANDS] = near[plane(7), :]
    xlo[BANDS] = near[plane(0), :]
    yhi[BANDS] = near[pl.ds(7, 8, stride=8), :]
    ylo[BANDS] = near[pl.ds(0, 8, stride=8), :]


def second_image(
    middle, inverse, lane_middle, lane_inverse, orb, pot, first, xm, xp, ym, yp, zm, zp, zhi, zlo,
    second, coarse, mhi, mlo, edge,
):
    lane, row = lanes(), rows()
    even_lane, even_row = (lane & 1) == 0, (row & 1) == 0

    cells = [nearest(lane, zp, zm, x) for x in range(8)]
    pots = nearest(lane, zp, zm, 8)
    for x in range(8):
        v = cells[x]
        outer = jnp.where(even_lane, lroll(zp[x], 127), lroll(zm[x], 1))
        inner = jnp.where(even_lane, lroll(zhi[x], 127), lroll(zlo[x], 1))
        left = cells[x - 1] if x > 0 else xm[BANDS]
        right = cells[x + 1] if x < 7 else xp[BANDS]
        up = jnp.where(row == 7, yp[BANDS, pl.ds(x, 1), :], sroll(v, 7))
        down = jnp.where(row == 0, ym[BANDS, pl.ds(x, 1), :], sroll(v, 1))
        total = (left + right) + (up + down) + (outer + inner)
        here = jnp.where(even_lane, pots[:, 2 * x : 2 * x + 1], pots[:, 2 * x + 1 : 2 * x + 2])
        edge[plane(x), :] = ((3.0 - lane_middle[...] + here) * v - 0.5 * total) * lane_inverse[...]

    def image(b, x):
        get = lambda i: first[b, plane(i), :]
        v = get(x)
        total = star(v, x, b, get, xm, xp, ym, yp, edge[plane(x), :], lane, row)
        c, r = middle[b], inverse[b]
        value = (((3.0 - c) + pot[plane(x), :]) * v - 0.5 * total) * (2.0 * r)
        value = value - orb[b, plane(x), :]
        second[b, plane(x), :] = value
        return value

    def pair_lanes(a, b):
        return jnp.where(even_lane, a + lroll(a, 127), b + lroll(b, 1))

    def pair_rows(a, b):
        return jnp.where(even_row, a + sroll(a, 7), b + sroll(b, 1))

    def group(g, _):
        odd = g & 1
        for big in range(4):
            sums = []
            for k in range(4):
                b = g * 4 + k
                sums.append(image(b, 2 * big) + image(b, 2 * big + 1))
            packed = 0.5 * pair_rows(pair_lanes(sums[0], sums[1]), pair_lanes(sums[2], sums[3]))
            coarse[g, plane(big), :] = packed
            mine = (lane >> 4) == 2 * big + odd
            at = 32 * big + 16 * odd
            half = g >> 1
            mhi[half] = jnp.where(mine, lroll(packed, (at + 16) & 127), mhi[half])
            mlo[half] = jnp.where(mine, lroll(packed, at), mlo[half])
        return 0

    sums = [pot[plane(2 * i), :] + pot[plane(2 * i + 1), :] for i in range(4)]
    packed = 0.125 * pair_rows(pair_lanes(sums[0], sums[1]), pair_lanes(sums[2], sums[3]))
    mhi[8] = packed
    mlo[8] = packed
    lax.fori_loop(0, GROUPS, group, 0)
    for g in range(GROUPS):
        coarse[g, plane(4), :] = packed


def add_halo(left, right, coarse_in, coarse):
    lane = lanes()
    first_half = ((lane >> 4) & 1) == 0
    beyond = jnp.where(lane < 64, right[8], left[8])
    for g in range(GROUPS):
        a, b = left[g // 2], right[g // 2]
        if g % 2 == 0:
            b = lroll(b, 16)
        else:
            a = lroll(a, 112)
        coarse[g, plane(5), :] = jnp.where(first_half, a, b)
        coarse[g, plane(6), :] = beyond


def coarse_solve(got, out, source, diagonal, scale, start, level, source_two, scale_two, two_a, two_b):
    lane, row = lanes(), rows()
    even_lane, even_row = (lane & 1) == 0, (row & 1) == 0
    low_lane, low_row = (lane & 2) == 0, (row & 2) == 0

    def pair_sum(v):
        v = v + jnp.where(low_row, sroll(v, 6), sroll(v, 2))
        return v + jnp.where(low_lane, lroll(v, 126), lroll(v, 2))

    def spread(v):
        a = jnp.where(even_lane, v, lroll(v, 1))
        b = jnp.where(even_lane, lroll(v, 127), v)
        out = []
        for w in (a, b):
            out.append((jnp.where(even_row, w, sroll(w, 1)), jnp.where(even_row, sroll(w, 7), w)))
        return [out[0][0], out[1][0], out[0][1], out[1][1]]

    def unpack(src, _):
        gx, gy = src >> 2, src & 3
        halo = got[src, plane(5), :]
        for t in range(2):
            pots = spread(got[src, plane(4 if t == 0 else 6), :])
            for big in range(4):
                at = (gx * 4 + big, gy * 2 + t)
                b = got[src, plane(big), :] if t == 0 else lroll(halo, 112 - 32 * big)
                d = pots[big] + 0.8
                w = weight / d
                source[at] = b
                diagonal[at] = d
                scale[at] = 0.125 * w
                start[at] = w * b
            for k in range(2):
                p = 0.125 * pair_sum(pots[2 * k] + pots[2 * k + 1])
                scale_two[gx * 2 + k, gy * 2 + t] = weight / (p + 0.2375)
        return 0

    lax.fori_loop(0, GROUPS, unpack, 0)

    def load(ref, x):
        return [[ref[x, gy * 2 + t] for t in range(2)] for gy in range(4)]

    def sides(ref, x, count, step, only=2):
        here = load(ref, x)
        before = lax.rem(x + (count - 1), count)
        after = lax.rem(x + 1, count)
        down = [[sroll(here[gy][t], step) for t in range(2)] for gy in range(4)]
        up = [[sroll(here[gy][t], 8 - step) for t in range(2)] for gy in range(4)] if step != 4 else down
        behind = [[lroll(here[gy][t], step) for t in range(2)] for gy in range(4)]
        ahead = [[lroll(here[gy][t], 128 - step) for t in range(2)] for gy in range(4)]
        totals = []
        for gy in range(4):
            line = []
            for t in range(only):
                total = ref[before, gy * 2 + t] + ref[after, gy * 2 + t]
                y = jnp.where(row < step, down[(gy + 3) % 4][t], down[gy][t])
                y = y + jnp.where(row >= 8 - step, up[(gy + 1) % 4][t], up[gy][t])
                z = jnp.where(lane < step, behind[gy][1 - t], behind[gy][t])
                z = z + jnp.where(lane >= 128 - step, ahead[gy][1 - t], ahead[gy][t])
                line.append(total + y + z)
            totals.append(line)
        return here, totals

    def sweep_one(x, _):
        here, totals = sides(start, x, 16, 2)
        for gy in range(4):
            for t in range(2):
                at = (x, gy * 2 + t)
                level[at] = (4.0 / 3.0) * here[gy][t] + scale[at] * totals[gy][t]
        return 0

    lax.fori_loop(0, 16, sweep_one, 0)

    def residue(pair, _):
        sums = [[None, None] for _ in range(4)]
        for k in range(2):
            x = 2 * pair + k
            here, totals = sides(level, x, 16, 2)
            for gy in range(4):
                for t in range(2):
                    at = (x, gy * 2 + t)
                    r = source[at] - (diagonal[at] * here[gy][t] - 0.125 * totals[gy][t])
                    sums[gy][t] = r if k == 0 else sums[gy][t] + r
        for gy in range(4):
            for t in range(2):
                at = (pair, gy * 2 + t)
                source_two[at] = scale_two[at] * (0.5 * pair_sum(sums[gy][t]))
        return 0

    lax.fori_loop(0, 8, residue, 0)

    def sweep_two(old, new):
        def body(x, _):
            here, totals = sides(old, x, 8, 4)
            for gy in range(4):
                for t in range(2):
                    at = (x, gy * 2 + t)
                    new[at] = (
                        (1.0 / 3.0) * here[gy][t]
                        + source_two[at]
                        + (0.03125 * scale_two[at]) * totals[gy][t]
                    )
            return 0

        lax.fori_loop(0, 8, body, 0)

    sweep_two(source_two, two_a)
    sweep_two(two_a, two_b)

    def correct(pair, _):
        for k in range(2):
            for i in range(8):
                at = (2 * pair + k, i)
                level[at] = level[at] + two_b[pair, i]
        return 0

    lax.fori_loop(0, 8, correct, 0)

    def last(x, _):
        here, totals = sides(level, x, 16, 2, only=1)
        gx, big = x >> 2, x & 3
        for gy in range(4):
            at = (x, gy * 2)
            value = (1.0 / 3.0) * here[gy][0] + start[at] + scale[at] * totals[gy][0]
            out[gx * 4 + gy, pl.ds(pl.multiple_of(big * 8, 8), 8), :] = value
        return 0

    lax.fori_loop(0, 16, last, 0)


def finish(second, got, out):
    lane, row = lanes(), rows()
    even_lane, even_row = (lane & 1) == 0, (row & 1) == 0

    def group(g, _):
        for big in range(4):
            v = got[g, plane(big), :]
            pair = (
                jnp.where(even_lane, v, lroll(v, 1)),
                jnp.where(even_lane, lroll(v, 127), v),
            )
            for k in range(4):
                w = pair[k % 2]
                if k < 2:
                    w = jnp.where(even_row, w, sroll(w, 1))
                else:
                    w = jnp.where(even_row, sroll(w, 7), w)
                b = g * 4 + k
                for x in (2 * big, 2 * big + 1):
                    out[b, plane(x), :] = second[b, plane(x), :] + w
        return 0

    lax.fori_loop(0, GROUPS, group, 0)


def swap(high, low, axis):
    size = lax.axis_size(axis)
    up = [(i, (i + 1) % size) for i in range(size)]
    return lax.ppermute(high, axis, up), lax.ppermute(low, axis, [(b, a) for a, b in up])


def local(orbitals, potential, centre, half_width):
    orb = orbitals.reshape(BANDS, 64, 128)
    pot = potential.reshape(64, 128)
    inverse = 1.0 / half_width
    lane_middle = jnp.repeat(centre, 2)[None]
    lane_inverse = jnp.repeat(inverse, 2)[None]
    face, wide = shape(BANDS, 8, 128), shape(BANDS + 1, 8, 128)
    thin, block = shape(9, 8, 128), shape(BANDS, 64, 128)

    xhi, xlo, yhi, ylo, zhi, zlo = call(
        pack_fine, [VMEM] * 2, (face, face, face, face, thin, thin)
    )(orb, pot)
    zm, zp = swap(zhi, zlo, "gz")
    ym, yp = swap(yhi, ylo, "gy")
    xm, xp = swap(xhi, xlo, "gx")
    first, xhi, xlo, yhi, ylo = call(
        first_image,
        [SMEM] * 2 + [VMEM] * 8,
        (block, wide, wide, wide, wide),
        scratch=(pltpu.VMEM((64, 128), jnp.float32),),
    )(centre, inverse, orb, pot, xm, xp, ym, yp, zm, zp)
    ym, yp = swap(yhi, ylo, "gy")
    xm, xp = swap(xhi, xlo, "gx")
    second, coarse, mhi, mlo = call(
        second_image,
        [SMEM] * 2 + [VMEM] * 13,
        (block, shape(GROUPS, 56, 128), thin, thin),
        scratch=(pltpu.VMEM((64, 128), jnp.float32),),
    )(centre, inverse, lane_middle, lane_inverse, orb, pot, first, xm, xp, ym, yp, zm, zp, zhi, zlo)
    left, right = swap(mhi, mlo, "gz")
    (coarse,) = call(add_halo, [VMEM] * 3, (shape(GROUPS, 56, 128),), aliases={2: 0})(
        left, right, coarse
    )
    got = lax.all_to_all(coarse, ("gx", "gy"), 0, 0, tiled=True)
    lines = pltpu.VMEM((16, 8, 8, 128), jnp.float32)
    half = pltpu.VMEM((8, 8, 8, 128), jnp.float32)
    (level,) = call(
        coarse_solve,
        [VMEM],
        (shape(GROUPS, 32, 128),),
        scratch=(lines,) * 5 + (half,) * 4,
    )(got)
    level = lax.all_to_all(level, ("gx", "gy"), 0, 0, tiled=True)
    (out,) = call(finish, [VMEM] * 2, (block,))(second, level)
    return out.reshape(BANDS, 8, 8, 128)


def solution(mesh):
    in_specs = (P(None, "gx", "gy", "gz"), P("gx", "gy", "gz"), P(), P())
    out_specs = P(None, "gx", "gy", "gz")
    return jax.shard_map(local, mesh=mesh, in_specs=in_specs, out_specs=out_specs, check_vma=False)
```

```python
import jax
import jax.numpy as jnp
from jax import lax
from jax.experimental import pallas as pl
from jax.experimental.pallas import tpu as pltpu
from jax.sharding import PartitionSpec as P

BANDS = 64
TILE = (8, 128)
GROUPS = 16
weight = 2.0 / 3.0

VMEM = pl.BlockSpec(memory_space=pltpu.VMEM)
SMEM = pl.BlockSpec(memory_space=pltpu.SMEM)
HBM = pl.BlockSpec(memory_space=pltpu.HBM)
CHUNKS = 8
BUSY = 400_000_000


def shape(*dims):
    return jax.ShapeDtypeStruct(dims, jnp.float32)


def call(body, ins, outs, scratch=(), aliases=None, flops=4_000_000, limit=2, out_specs=None):
    return pl.pallas_call(
        body,
        out_shape=outs,
        in_specs=ins,
        out_specs=out_specs or tuple(VMEM for _ in outs),
        scratch_shapes=scratch,
        input_output_aliases=aliases or {},
        compiler_params=pltpu.CompilerParams(vmem_limit_bytes=limit * 1024 * 1024),
        cost_estimate=pl.CostEstimate(flops=flops, bytes_accessed=4_000_000, transcendentals=0),
    )


def lanes():
    return lax.broadcasted_iota(jnp.int32, TILE, 1)


def rows():
    return lax.broadcasted_iota(jnp.int32, TILE, 0)


def lroll(v, shift):
    return pltpu.roll(v, shift, 1)


def sroll(v, shift):
    return pltpu.roll(v, shift, 0)


def plane(x):
    return pl.ds(x * 8, 8)


def loop(count, step, body):
    def several(i, _):
        for k in range(step):
            body(i * step + k, 0)
        return 0

    lax.fori_loop(0, count // step, several, 0)


def nearest(lane, zp, zm, x):
    return jnp.where((lane & 1) == 0, zp[x], zm[x])


def pack_fine(orb_hbm, pot_hbm, orb, xhi, xlo, yhi, ylo, zhi, zlo, pot, sems):
    lane = lanes()
    pot_copy = pltpu.make_async_copy(pot_hbm, pot, sems.at[CHUNKS])
    pot_copy.start()
    copies = []
    for i in range(CHUNKS):
        part = pl.ds(i * (BANDS // CHUNKS), BANDS // CHUNKS)
        copies.append(pltpu.make_async_copy(orb_hbm.at[part], orb.at[part], sems.at[i]))
        copies[i].start()

    def put(carry, v, slot):
        high, low = carry
        turned = lroll(v, (2 * slot + 2) & 127)
        high = jnp.where((lane >> 1) == slot, turned, high)
        low = jnp.where((lane >> 1) == ((slot + 1) & 63), turned, low)
        return high, low

    zero = jnp.zeros(TILE, jnp.float32)
    step = 4

    def body(i, carry):
        carry = list(carry)
        for k in range(step):
            b = i * step + k
            for x in range(8):
                v = orb[b, plane(x), :]
                carry[x] = put(carry[x], v, b)
                if x == 7:
                    xhi[b] = v
                if x == 0:
                    xlo[b] = v
            yhi[b] = orb[b, pl.ds(7, 8, stride=8), :]
            ylo[b] = orb[b, pl.ds(0, 8, stride=8), :]
        return tuple(carry)

    carry = tuple((zero, zero) for _ in range(8))
    each = BANDS // CHUNKS // step
    for i in range(CHUNKS):
        copies[i].wait()
        carry = lax.fori_loop(i * each, (i + 1) * each, body, carry)
    for x in range(8):
        zhi[x] = carry[x][0]
        zlo[x] = lroll(carry[x][1], 126)
    pot_copy.wait()
    edge = (zero, zero)
    for x in range(8):
        edge = put(edge, pot[plane(x), :], x)
    zhi[8] = edge[0]
    zlo[8] = lroll(edge[1], 126)


def inner_sum(get, x, lane, row):
    v = get(x)
    up = jnp.where(row == 7, 0.0, sroll(v, 7))
    down = jnp.where(row == 0, 0.0, sroll(v, 1))
    ahead = jnp.where(lane == 127, 0.0, lroll(v, 127))
    behind = jnp.where(lane == 0, 0.0, lroll(v, 1))
    total = (up + down) + (ahead + behind)
    if x > 0:
        total = total + get(x - 1)
    if x < 7:
        total = total + get(x + 1)
    return v, total


def outer_sum(x, b, xm, xp, ym, yp, halo, ends, row):
    total = jnp.where(ends, lroll(halo, 127 - 2 * b), 0.0)
    y = jnp.where(row == 0, ym[b, pl.ds(x, 1), :], yp[b, pl.ds(x, 1), :])
    total = total + jnp.where((row == 0) | (row == 7), y, 0.0)
    if x == 0:
        total = total + xm[b]
    if x == 7:
        total = total + xp[b]
    return total


def first_inside(middle, inverse, orb, pot, first, by_lane):
    lane, row = lanes(), rows()
    step = 4

    def body(i, carry):
        lane_c, lane_r = carry
        for k in range(step):
            b = i * step + k
            c, r = middle[b], inverse[b]
            lane_c = jnp.where((lane >> 1) == b, c, lane_c)
            lane_r = jnp.where((lane >> 1) == b, r, lane_r)
            get = lambda x: orb[b, plane(x), :]
            for x in range(8):
                v, total = inner_sum(get, x, lane, row)
                first[b, plane(x), :] = (((3.0 - c) + pot[plane(x), :]) * v - 0.5 * total) * r
        return lane_c, lane_r

    zero = jnp.zeros(TILE, jnp.float32)
    by_lane[0], by_lane[1] = lax.fori_loop(0, BANDS // step, body, (zero, zero))


def first_edges(inverse, part, xm, xp, ym, yp, zm, zp, first, xhi, xlo, yhi, ylo, near):
    lane, row = lanes(), rows()
    ends = (lane == 0) | (lane == 127)
    for x in range(8):
        near[plane(x), :] = nearest(lane, zp, zm, x)
    step = 4

    def body(i, _):
        values = []
        for k in range(step):
            b = i * step + k
            r = -0.5 * inverse[b]
            for x in range(8):
                total = outer_sum(x, b, xm, xp, ym, yp, near[plane(x), :], ends, row)
                values.append(part[b, plane(x), :] + r * total)
        for k in range(step):
            b = i * step + k
            for x in range(8):
                first[b, plane(x), :] = values[8 * k + x]
            xhi[b] = values[8 * k + 7]
            xlo[b] = values[8 * k]
        for k in range(step):
            b = i * step + k
            yhi[b] = first[b, pl.ds(7, 8, stride=8), :]
            ylo[b] = first[b, pl.ds(0, 8, stride=8), :]
        return 0

    lax.fori_loop(0, BANDS // step, body, 0)
    xhi[BANDS] = near[plane(7), :]
    xlo[BANDS] = near[plane(0), :]
    yhi[BANDS] = near[pl.ds(7, 8, stride=8), :]
    ylo[BANDS] = near[pl.ds(0, 8, stride=8), :]


def second_inside(middle, inverse, orb, pot, first, second):
    lane, row = lanes(), rows()
    step = 4

    def body(i, _):
        for k in range(step):
            b = i * step + k
            c, r = middle[b], 2.0 * inverse[b]
            get = lambda x: first[b, plane(x), :]
            for x in range(8):
                v, total = inner_sum(get, x, lane, row)
                value = (((3.0 - c) + pot[plane(x), :]) * v - 0.5 * total) * r
                second[b, plane(x), :] = value - orb[b, plane(x), :]
        return 0

    lax.fori_loop(0, BANDS // step, body, 0)


def second_edges(
    inverse, by_lane, pot, part, xm, xp, ym, yp, zm, zp, zhi, zlo,
    second, coarse, mhi, mlo, edge,
):
    lane, row = lanes(), rows()
    ends = (lane == 0) | (lane == 127)
    even_lane, even_row = (lane & 1) == 0, (row & 1) == 0

    cells = [nearest(lane, zp, zm, x) for x in range(8)]
    pots = nearest(lane, zp, zm, 8)
    for x in range(8):
        v = cells[x]
        outer = jnp.where(even_lane, lroll(zp[x], 127), lroll(zm[x], 1))
        inner = jnp.where(even_lane, lroll(zhi[x], 127), lroll(zlo[x], 1))
        left = cells[x - 1] if x > 0 else xm[BANDS]
        right = cells[x + 1] if x < 7 else xp[BANDS]
        up = jnp.where(row == 7, yp[BANDS, pl.ds(x, 1), :], sroll(v, 7))
        down = jnp.where(row == 0, ym[BANDS, pl.ds(x, 1), :], sroll(v, 1))
        total = (left + right) + (up + down) + (outer + inner)
        here = jnp.where(even_lane, pots[:, 2 * x : 2 * x + 1], pots[:, 2 * x + 1 : 2 * x + 2])
        edge[plane(x), :] = ((3.0 - by_lane[0] + here) * v - 0.5 * total) * by_lane[1]

    def image(b, x):
        total = outer_sum(x, b, xm, xp, ym, yp, edge[plane(x), :], ends, row)
        return part[b, plane(x), :] - inverse[b] * total

    def pair_lanes(a, b):
        return jnp.where(even_lane, a + lroll(a, 127), b + lroll(b, 1))

    def pair_rows(a, b):
        return jnp.where(even_row, a + sroll(a, 7), b + sroll(b, 1))

    def group(g, _):
        odd = g & 1
        half = g >> 1
        done, values = [], []
        for big in range(4):
            sums = []
            for k in range(4):
                b = g * 4 + k
                pair = image(b, 2 * big), image(b, 2 * big + 1)
                values.append((b, 2 * big, pair[0]))
                values.append((b, 2 * big + 1, pair[1]))
                sums.append(pair[0] + pair[1])
            done.append(0.5 * pair_rows(pair_lanes(sums[0], sums[1]), pair_lanes(sums[2], sums[3])))
        for b, x, value in values:
            second[b, plane(x), :] = value
        high, low = mhi[half], mlo[half]
        for big in range(4):
            coarse[g, plane(big), :] = done[big]
            mine = (lane >> 4) == 2 * big + odd
            at = 32 * big + 16 * odd
            high = jnp.where(mine, lroll(done[big], (at + 16) & 127), high)
            low = jnp.where(mine, lroll(done[big], at), low)
        mhi[half] = high
        mlo[half] = low
        return 0

    sums = [pot[plane(2 * i), :] + pot[plane(2 * i + 1), :] for i in range(4)]
    packed = 0.125 * pair_rows(pair_lanes(sums[0], sums[1]), pair_lanes(sums[2], sums[3]))
    mhi[8] = packed
    mlo[8] = packed
    lax.fori_loop(0, GROUPS, group, 0)
    for g in range(GROUPS):
        coarse[g, plane(4), :] = packed


def add_halo(left, right, coarse_in, coarse):
    lane = lanes()
    first_half = ((lane >> 4) & 1) == 0
    beyond = jnp.where(lane < 64, right[8], left[8])
    for g in range(GROUPS):
        a, b = left[g // 2], right[g // 2]
        if g % 2 == 0:
            b = lroll(b, 16)
        else:
            a = lroll(a, 112)
        coarse[g, plane(5), :] = jnp.where(first_half, a, b)
        coarse[g, plane(6), :] = beyond


def coarse_solve(got, out, source, diagonal, scale, start, level, source_two, scale_two, two_a, two_b):
    lane, row = lanes(), rows()
    even_lane, even_row = (lane & 1) == 0, (row & 1) == 0
    low_lane, low_row = (lane & 2) == 0, (row & 2) == 0

    def pair_sum(v):
        v = v + jnp.where(low_row, sroll(v, 6), sroll(v, 2))
        return v + jnp.where(low_lane, lroll(v, 126), lroll(v, 2))

    def spread(v):
        a = jnp.where(even_lane, v, lroll(v, 1))
        b = jnp.where(even_lane, lroll(v, 127), v)
        out = []
        for w in (a, b):
            out.append((jnp.where(even_row, w, sroll(w, 1)), jnp.where(even_row, sroll(w, 7), w)))
        return [out[0][0], out[1][0], out[0][1], out[1][1]]

    def unpack(src, _):
        gx, gy = src >> 2, src & 3
        halo = got[src, plane(5), :]
        for t in range(2):
            pots = spread(got[src, plane(4 if t == 0 else 6), :])
            for big in range(4):
                at = (gx * 4 + big, gy * 2 + t)
                b = got[src, plane(big), :] if t == 0 else lroll(halo, 112 - 32 * big)
                d = pots[big] + 0.8
                w = weight / d
                source[at] = b
                diagonal[at] = d
                scale[at] = 0.125 * w
                start[at] = w * b
            for k in range(2):
                p = 0.125 * pair_sum(pots[2 * k] + pots[2 * k + 1])
                scale_two[gx * 2 + k, gy * 2 + t] = weight / (p + 0.2375)
        return 0

    loop(GROUPS, 2, unpack)

    def load(ref, x):
        return [[ref[x, gy * 2 + t] for t in range(2)] for gy in range(4)]

    def sides(ref, x, count, step, only=2):
        here = load(ref, x)
        before = lax.rem(x + (count - 1), count)
        after = lax.rem(x + 1, count)
        down = [[sroll(here[gy][t], step) for t in range(2)] for gy in range(4)]
        up = [[sroll(here[gy][t], 8 - step) for t in range(2)] for gy in range(4)] if step != 4 else down
        behind = [[lroll(here[gy][t], step) for t in range(2)] for gy in range(4)]
        ahead = [[lroll(here[gy][t], 128 - step) for t in range(2)] for gy in range(4)]
        totals = []
        for gy in range(4):
            line = []
            for t in range(only):
                total = ref[before, gy * 2 + t] + ref[after, gy * 2 + t]
                y = jnp.where(row < step, down[(gy + 3) % 4][t], down[gy][t])
                y = y + jnp.where(row >= 8 - step, up[(gy + 1) % 4][t], up[gy][t])
                z = jnp.where(lane < step, behind[gy][1 - t], behind[gy][t])
                z = z + jnp.where(lane >= 128 - step, ahead[gy][1 - t], ahead[gy][t])
                line.append(total + y + z)
            totals.append(line)
        return here, totals

    def sweep_one(x, _):
        here, totals = sides(start, x, 16, 2)
        for gy in range(4):
            for t in range(2):
                at = (x, gy * 2 + t)
                level[at] = (4.0 / 3.0) * here[gy][t] + scale[at] * totals[gy][t]
        return 0

    loop(16, 4, sweep_one)

    def residue(pair, _):
        sums = [[None, None] for _ in range(4)]
        for k in range(2):
            x = 2 * pair + k
            here, totals = sides(level, x, 16, 2)
            for gy in range(4):
                for t in range(2):
                    at = (x, gy * 2 + t)
                    r = source[at] - (diagonal[at] * here[gy][t] - 0.125 * totals[gy][t])
                    sums[gy][t] = r if k == 0 else sums[gy][t] + r
        for gy in range(4):
            for t in range(2):
                at = (pair, gy * 2 + t)
                source_two[at] = scale_two[at] * (0.5 * pair_sum(sums[gy][t]))
        return 0

    loop(8, 2, residue)

    def sweep_two(old, new):
        def body(x, _):
            here, totals = sides(old, x, 8, 4)
            for gy in range(4):
                for t in range(2):
                    at = (x, gy * 2 + t)
                    new[at] = (
                        (1.0 / 3.0) * here[gy][t]
                        + source_two[at]
                        + (0.03125 * scale_two[at]) * totals[gy][t]
                    )
            return 0

        loop(8, 4, body)

    sweep_two(source_two, two_a)
    sweep_two(two_a, two_b)

    def correct(pair, _):
        for k in range(2):
            for i in range(8):
                at = (2 * pair + k, i)
                level[at] = level[at] + two_b[pair, i]
        return 0

    loop(8, 4, correct)

    def last(x, _):
        here, totals = sides(level, x, 16, 2, only=1)
        gx, big = x >> 2, x & 3
        for gy in range(4):
            at = (x, gy * 2)
            value = (1.0 / 3.0) * here[gy][0] + start[at] + scale[at] * totals[gy][0]
            out[gx * 4 + gy, pl.ds(pl.multiple_of(big * 8, 8), 8), :] = value
        return 0

    loop(16, 4, last)


def finish(second, got, out_hbm, out, sems):
    lane, row = lanes(), rows()
    even_lane, even_row = (lane & 1) == 0, (row & 1) == 0

    def group(g, _):
        for big in range(4):
            v = got[g, plane(big), :]
            pair = (
                jnp.where(even_lane, v, lroll(v, 1)),
                jnp.where(even_lane, lroll(v, 127), v),
            )
            for k in range(4):
                w = pair[k % 2]
                if k < 2:
                    w = jnp.where(even_row, w, sroll(w, 1))
                else:
                    w = jnp.where(even_row, sroll(w, 7), w)
                b = g * 4 + k
                for x in (2 * big, 2 * big + 1):
                    out[b, plane(x), :] = second[b, plane(x), :] + w
        return 0

    copies = []
    each = GROUPS // CHUNKS
    for i in range(CHUNKS):
        for g in range(i * each, (i + 1) * each):
            group(g, 0)
        part = pl.ds(i * (BANDS // CHUNKS), BANDS // CHUNKS)
        copies.append(pltpu.make_async_copy(out.at[part], out_hbm.at[part], sems.at[i]))
        copies[i].start()
    for copy in copies:
        copy.wait()


def swap(high, low, axis):
    size = lax.axis_size(axis)
    up = [(i, (i + 1) % size) for i in range(size)]
    return lax.ppermute(high, axis, up), lax.ppermute(low, axis, [(b, a) for a, b in up])


def in_hbm(array):
    return pltpu.with_memory_space_constraint(array, pltpu.HBM)


def local(orbitals, potential, centre, half_width):
    orb = orbitals.reshape(BANDS, 64, 128)
    pot = potential.reshape(64, 128)
    inverse = 1.0 / half_width
    face, wide = shape(BANDS, 8, 128), shape(BANDS + 1, 8, 128)
    thin, block = shape(9, 8, 128), shape(BANDS, 64, 128)

    orb, xhi, xlo, yhi, ylo, zhi, zlo = call(
        pack_fine,
        [HBM, HBM],
        (block, face, face, face, face, thin, thin),
        scratch=(pltpu.VMEM((64, 128), jnp.float32), pltpu.SemaphoreType.DMA((CHUNKS + 1,))),
    )(in_hbm(orb), in_hbm(pot))
    zm, zp = swap(zhi, zlo, "gz")
    ym, yp = swap(yhi, ylo, "gy")
    xm, xp = swap(xhi, xlo, "gx")
    part, by_lane = call(
        first_inside, [SMEM] * 2 + [VMEM] * 2, (block, shape(2, 8, 128)), flops=BUSY
    )(centre, inverse, orb, pot)
    near = (pltpu.VMEM((64, 128), jnp.float32),)
    first, xhi, xlo, yhi, ylo = call(
        first_edges, [SMEM] + [VMEM] * 7, (block, wide, wide, wide, wide), scratch=near
    )(inverse, part, xm, xp, ym, yp, zm, zp)
    ym, yp = swap(yhi, ylo, "gy")
    xm, xp = swap(xhi, xlo, "gx")
    (part,) = call(second_inside, [SMEM] * 2 + [VMEM] * 3, (block,), flops=BUSY)(
        centre, inverse, orb, pot, first
    )
    second, coarse, mhi, mlo = call(
        second_edges,
        [SMEM] + [VMEM] * 11,
        (block, shape(GROUPS, 56, 128), thin, thin),
        scratch=near,
    )(inverse, by_lane, pot, part, xm, xp, ym, yp, zm, zp, zhi, zlo)
    left, right = swap(mhi, mlo, "gz")
    (coarse,) = call(add_halo, [VMEM] * 3, (shape(GROUPS, 56, 128),), aliases={2: 0})(
        left, right, coarse
    )
    got = lax.all_to_all(coarse, ("gx", "gy"), 0, 0, tiled=True)
    lines = pltpu.VMEM((16, 8, 8, 128), jnp.float32)
    half = pltpu.VMEM((8, 8, 8, 128), jnp.float32)
    (level,) = call(
        coarse_solve,
        [VMEM],
        (shape(GROUPS, 32, 128),),
        scratch=(lines,) * 5 + (half,) * 4,
        limit=6,
    )(got)
    level = lax.all_to_all(level, ("gx", "gy"), 0, 0, tiled=True)
    (out,) = call(
        finish,
        [VMEM] * 2,
        (block,),
        out_specs=(HBM,),
        scratch=(pltpu.VMEM((BANDS, 64, 128), jnp.float32), pltpu.SemaphoreType.DMA((CHUNKS,))),
        limit=4,
    )(second, level)
    return out.reshape(BANDS, 8, 8, 128)


def solution(mesh):
    in_specs = (P(None, "gx", "gy", "gz"), P("gx", "gy", "gz"), P(), P())
    out_specs = P(None, "gx", "gy", "gz")
    return jax.shard_map(local, mesh=mesh, in_specs=in_specs, out_specs=out_specs, check_vma=False)
```

```python
import jax
import jax.numpy as jnp
from jax import lax
from jax.experimental import pallas as pl
from jax.experimental.pallas import tpu as pltpu
from jax.sharding import PartitionSpec as P

BANDS = 64
TILE = (8, 128)
GROUPS = 16
weight = 2.0 / 3.0

VMEM = pl.BlockSpec(memory_space=pltpu.VMEM)
SMEM = pl.BlockSpec(memory_space=pltpu.SMEM)
HBM = pl.BlockSpec(memory_space=pltpu.HBM)
CHUNKS = 4
BUSY = 400_000_000
T_FIRST, T_INSIDE, T_EDGE, T_SECOND, T_PACK, T_SEND = 16, 16, 32, 32, 16, 8
T_OPEN, T_SWEEP, T_REST, T_TWO, T_LAST = 8, 16, 8, 8, 16


def shape(*dims):
    return jax.ShapeDtypeStruct(dims, jnp.float32)


def call(body, ins, outs, scratch=(), aliases=None, flops=4_000_000, limit=2, out_specs=None):
    return pl.pallas_call(
        body,
        out_shape=outs,
        in_specs=ins,
        out_specs=out_specs or tuple(VMEM for _ in outs),
        scratch_shapes=scratch,
        input_output_aliases=aliases or {},
        compiler_params=pltpu.CompilerParams(vmem_limit_bytes=limit * 1024 * 1024),
        cost_estimate=pl.CostEstimate(flops=flops, bytes_accessed=4_000_000, transcendentals=0),
    )


def lanes():
    return lax.broadcasted_iota(jnp.int32, TILE, 1)


def rows():
    return lax.broadcasted_iota(jnp.int32, TILE, 0)


def lroll(v, shift):
    return pltpu.roll(v, shift, 1)


def sroll(v, shift):
    return pltpu.roll(v, shift, 0)


def plane(x):
    return pl.ds(x * 8, 8)


def loop(count, step, body):
    def several(i, _):
        for k in range(step):
            body(i * step + k, 0)
        return 0

    lax.fori_loop(0, count // step, several, 0)


def nearest(lane, zp, zm, x):
    return jnp.where((lane & 1) == 0, zp[x], zm[x])


def pack_fine(orb_hbm, pot_hbm, orb, xhi, xlo, yhi, ylo, zhi, zlo, pot, sems):
    lane = lanes()
    pot_copy = pltpu.make_async_copy(pot_hbm, pot, sems.at[CHUNKS])
    pot_copy.start()
    copies = []
    for i in range(CHUNKS):
        part = pl.ds(i * (BANDS // CHUNKS), BANDS // CHUNKS)
        copies.append(pltpu.make_async_copy(orb_hbm.at[part], orb.at[part], sems.at[i]))
        copies[i].start()

    def put(carry, v, slot):
        high, low = carry
        turned = lroll(v, (2 * slot + 2) & 127)
        high = jnp.where((lane >> 1) == slot, turned, high)
        low = jnp.where((lane >> 1) == ((slot + 1) & 63), turned, low)
        return high, low

    zero = jnp.zeros(TILE, jnp.float32)
    step = T_FIRST

    def body(i, carry):
        carry = list(carry)
        for k in range(step):
            b = i * step + k
            for x in range(8):
                v = orb[b, plane(x), :]
                carry[x] = put(carry[x], v, b)
                if x == 7:
                    xhi[b] = v
                if x == 0:
                    xlo[b] = v
            yhi[b] = orb[b, pl.ds(7, 8, stride=8), :]
            ylo[b] = orb[b, pl.ds(0, 8, stride=8), :]
        return tuple(carry)

    carry = tuple((zero, zero) for _ in range(8))
    each = BANDS // CHUNKS // step
    for i in range(CHUNKS):
        copies[i].wait()
        carry = lax.fori_loop(i * each, (i + 1) * each, body, carry)
    for x in range(8):
        zhi[x] = carry[x][0]
        zlo[x] = lroll(carry[x][1], 126)
    pot_copy.wait()
    edge = (zero, zero)
    for x in range(8):
        edge = put(edge, pot[plane(x), :], x)
    zhi[8] = edge[0]
    zlo[8] = lroll(edge[1], 126)


def inner_sum(get, x, lane, row):
    v = get(x)
    up = jnp.where(row == 7, 0.0, sroll(v, 7))
    down = jnp.where(row == 0, 0.0, sroll(v, 1))
    ahead = jnp.where(lane == 127, 0.0, lroll(v, 127))
    behind = jnp.where(lane == 0, 0.0, lroll(v, 1))
    total = (up + down) + (ahead + behind)
    if x > 0:
        total = total + get(x - 1)
    if x < 7:
        total = total + get(x + 1)
    return v, total


def outer_sum(x, b, xm, xp, ym, yp, halo, ends, row):
    total = jnp.where(ends, lroll(halo, 127 - 2 * b), 0.0)
    y = jnp.where(row == 0, ym[b, pl.ds(x, 1), :], yp[b, pl.ds(x, 1), :])
    total = total + jnp.where((row == 0) | (row == 7), y, 0.0)
    if x == 0:
        total = total + xm[b]
    if x == 7:
        total = total + xp[b]
    return total


def first_inside(middle, inverse, orb, pot, first, by_lane):
    lane, row = lanes(), rows()
    step = T_INSIDE

    def body(i, carry):
        lane_c, lane_r = carry
        for k in range(step):
            b = i * step + k
            c, r = middle[b], inverse[b]
            lane_c = jnp.where((lane >> 1) == b, c, lane_c)
            lane_r = jnp.where((lane >> 1) == b, r, lane_r)
            get = lambda x: orb[b, plane(x), :]
            for x in range(8):
                v, total = inner_sum(get, x, lane, row)
                first[b, plane(x), :] = (((3.0 - c) + pot[plane(x), :]) * v - 0.5 * total) * r
        return lane_c, lane_r

    zero = jnp.zeros(TILE, jnp.float32)
    by_lane[0], by_lane[1] = lax.fori_loop(0, BANDS // step, body, (zero, zero))


def first_edges(inverse, part, xm, xp, ym, yp, zm, zp, first, xhi, xlo, yhi, ylo, near):
    lane, row = lanes(), rows()
    ends = (lane == 0) | (lane == 127)
    for x in range(8):
        near[plane(x), :] = nearest(lane, zp, zm, x)
    step = T_EDGE

    def body(i, _):
        for k in range(step):
            b = i * step + k
            r = -0.5 * inverse[b]
            for x in range(8):
                total = outer_sum(x, b, xm, xp, ym, yp, near[plane(x), :], ends, row)
                value = part[b, plane(x), :] + r * total
                first[b, plane(x), :] = value
                if x == 7:
                    xhi[b] = value
                if x == 0:
                    xlo[b] = value
        for k in range(step):
            b = i * step + k
            yhi[b] = first[b, pl.ds(7, 8, stride=8), :]
            ylo[b] = first[b, pl.ds(0, 8, stride=8), :]
        return 0

    lax.fori_loop(0, BANDS // step, body, 0)
    xhi[BANDS] = near[plane(7), :]
    xlo[BANDS] = near[plane(0), :]
    yhi[BANDS] = near[pl.ds(7, 8, stride=8), :]
    ylo[BANDS] = near[pl.ds(0, 8, stride=8), :]


def second_inside(middle, inverse, orb, pot, first, second):
    lane, row = lanes(), rows()
    step = T_INSIDE

    def body(i, _):
        for k in range(step):
            b = i * step + k
            c, r = middle[b], 2.0 * inverse[b]
            get = lambda x: first[b, plane(x), :]
            for x in range(8):
                v, total = inner_sum(get, x, lane, row)
                value = (((3.0 - c) + pot[plane(x), :]) * v - 0.5 * total) * r
                second[b, plane(x), :] = value - orb[b, plane(x), :]
        return 0

    lax.fori_loop(0, BANDS // step, body, 0)


def second_edges(
    inverse, by_lane, pot, part, xm, xp, ym, yp, zm, zp, zhi, zlo,
    second, coarse, edge, sums,
):
    lane, row = lanes(), rows()
    ends = (lane == 0) | (lane == 127)
    even_lane, even_row = (lane & 1) == 0, (row & 1) == 0

    cells = [nearest(lane, zp, zm, x) for x in range(8)]
    pots = nearest(lane, zp, zm, 8)
    for x in range(8):
        v = cells[x]
        outer = jnp.where(even_lane, lroll(zp[x], 127), lroll(zm[x], 1))
        inner = jnp.where(even_lane, lroll(zhi[x], 127), lroll(zlo[x], 1))
        left = cells[x - 1] if x > 0 else xm[BANDS]
        right = cells[x + 1] if x < 7 else xp[BANDS]
        up = jnp.where(row == 7, yp[BANDS, pl.ds(x, 1), :], sroll(v, 7))
        down = jnp.where(row == 0, ym[BANDS, pl.ds(x, 1), :], sroll(v, 1))
        total = (left + right) + (up + down) + (outer + inner)
        here = jnp.where(even_lane, pots[:, 2 * x : 2 * x + 1], pots[:, 2 * x + 1 : 2 * x + 2])
        edge[plane(x), :] = ((3.0 - by_lane[0] + here) * v - 0.5 * total) * by_lane[1]

    def image(i, _):
        for k in range(T_SECOND):
            b = i * T_SECOND + k
            r = inverse[b]
            for big in range(4):
                pair = []
                for x in (2 * big, 2 * big + 1):
                    total = outer_sum(x, b, xm, xp, ym, yp, edge[plane(x), :], ends, row)
                    pair.append(part[b, plane(x), :] - r * total)
                    second[b, plane(x), :] = pair[-1]
                sums[b, plane(big), :] = pair[0] + pair[1]
        return 0

    def pair_lanes(a, b):
        return jnp.where(even_lane, a + lroll(a, 127), b + lroll(b, 1))

    def pair_rows(a, b):
        return jnp.where(even_row, a + sroll(a, 7), b + sroll(b, 1))

    def pack(g, _):
        for big in range(4):
            v = [sums[g * 4 + k, plane(big), :] for k in range(4)]
            coarse[g, plane(big), :] = 0.5 * pair_rows(pair_lanes(v[0], v[1]), pair_lanes(v[2], v[3]))

    four = [pot[plane(2 * i), :] + pot[plane(2 * i + 1), :] for i in range(4)]
    packed = 0.125 * pair_rows(pair_lanes(four[0], four[1]), pair_lanes(four[2], four[3]))
    for g in range(GROUPS):
        coarse[g, plane(4), :] = packed
    lax.fori_loop(0, BANDS // T_SECOND, image, 0)
    loop(GROUPS, T_PACK, pack)


def pack_ends(got, mhi, mlo):
    lane = lanes()
    zero = jnp.zeros(TILE, jnp.float32)

    def send(half, _):
        high = low = zero
        for odd in range(2):
            for big in range(4):
                v = got[2 * half + odd, plane(big), :]
                mine = (lane >> 4) == 2 * big + odd
                at = 32 * big + 16 * odd
                high = jnp.where(mine, lroll(v, (at + 16) & 127), high)
                low = jnp.where(mine, lroll(v, at), low)
        mhi[half] = high
        mlo[half] = low

    loop(GROUPS // 2, T_SEND, send)
    for half in range(2):
        high = low = zero
        for i in range(8):
            v = got[8 * half + i, plane(4), :]
            high = jnp.where((lane >> 4) == i, lroll(v, (16 * i + 16) & 127), high)
            low = jnp.where((lane >> 4) == i, lroll(v, 16 * i), low)
        mhi[8 + half] = high
        mlo[8 + half] = low


def coarse_terms(blocks, pots, gx, gy, source, diagonal, scale, start, scale_two):
    lane, row = lanes(), rows()
    even_lane, even_row = (lane & 1) == 0, (row & 1) == 0
    a = jnp.where(even_lane, pots, lroll(pots, 1))
    b = jnp.where(even_lane, lroll(pots, 127), pots)
    each = []
    for up in (False, True):
        for w in (a, b):
            each.append(jnp.where(even_row, sroll(w, 7), w) if up else jnp.where(even_row, w, sroll(w, 1)))
    for big in range(4):
        at = (gx * 4 + big, gy)
        d = each[big] + 0.8
        w = weight / d
        source[at] = blocks[big]
        diagonal[at] = d
        scale[at] = 0.125 * w
        start[at] = w * blocks[big]
    for k in range(2):
        p = 0.125 * pair_sum(each[2 * k] + each[2 * k + 1], lane, row)
        scale_two[gx * 2 + k, gy] = weight / (p + 0.2375)


def pair_sum(v, lane, row):
    v = v + jnp.where((row & 2) == 0, sroll(v, 6), sroll(v, 2))
    return v + jnp.where((lane & 2) == 0, lroll(v, 126), lroll(v, 2))


def open_block(got, source, diagonal, scale, start, scale_two):
    def unpack(src, _):
        blocks = [got[src, plane(big), :] for big in range(4)]
        pots = got[src, plane(4), :]
        coarse_terms(blocks, pots, src >> 2, src & 3, source, diagonal, scale, start, scale_two)

    loop(GROUPS, T_OPEN, unpack)


def coarse_solve(
    left, right, source_0, diagonal_0, scale_0, start_0, scale_two_0, out,
    source_1, diagonal_1, scale_1, start_1, scale_two_1,
    level_0, level_1, source_two_0, source_two_1, two_a_0, two_a_1, two_b_0, two_b_1,
):
    lane, row = lanes(), rows()
    source, diagonal = (source_0, source_1), (diagonal_0, diagonal_1)
    scale, start = (scale_0, scale_1), (start_0, start_1)
    scale_two, level = (scale_two_0, scale_two_1), (level_0, level_1)
    source_two, two_a, two_b = (
        (source_two_0, source_two_1),
        (two_a_0, two_a_1),
        (two_b_0, two_b_1),
    )

    def unpack(group, _):
        for i in range(8):
            src = 8 * group + i
            a, b = left[4 * group + i // 2], right[4 * group + i // 2]
            if i % 2 == 0:
                b = lroll(b, 16)
            else:
                a = lroll(a, 112)
            halo = jnp.where(((lane >> 4) & 1) == 0, a, b)
            blocks = [lroll(halo, 112 - 32 * big) for big in range(4)]
            near, far = right[8 + group], left[8 + group]
            pots = jnp.where(lane < 64, lroll(near, (128 - 16 * i) & 127), lroll(far, 112 - 16 * i))
            coarse_terms(
                blocks, pots, 2 * group + i // 4, i % 4,
                source_1, diagonal_1, scale_1, start_1, scale_two_1,
            )

    loop(2, 1, unpack)

    def load(ref, x):
        return [[ref[t][x, gy] for t in range(2)] for gy in range(4)]

    def sides(ref, x, count, step, only=2):
        here = load(ref, x)
        before = lax.rem(x + (count - 1), count)
        after = lax.rem(x + 1, count)
        down = [[sroll(here[gy][t], step) for t in range(2)] for gy in range(4)]
        up = [[sroll(here[gy][t], 8 - step) for t in range(2)] for gy in range(4)] if step != 4 else down
        behind = [[lroll(here[gy][t], step) for t in range(2)] for gy in range(4)]
        ahead = [[lroll(here[gy][t], 128 - step) for t in range(2)] for gy in range(4)]
        totals = []
        for gy in range(4):
            line = []
            for t in range(only):
                total = ref[t][before, gy] + ref[t][after, gy]
                y = jnp.where(row < step, down[(gy + 3) % 4][t], down[gy][t])
                y = y + jnp.where(row >= 8 - step, up[(gy + 1) % 4][t], up[gy][t])
                z = jnp.where(lane < step, behind[gy][1 - t], behind[gy][t])
                z = z + jnp.where(lane >= 128 - step, ahead[gy][1 - t], ahead[gy][t])
                line.append(total + y + z)
            totals.append(line)
        return here, totals

    def sweep_one(x, _):
        here, totals = sides(start, x, 16, 2)
        for gy in range(4):
            for t in range(2):
                value = (4.0 / 3.0) * here[gy][t] + scale[t][x, gy] * totals[gy][t]
                level[t][x, gy] = value

    loop(16, T_SWEEP, sweep_one)

    def residue(pair, _):
        sums = [[None, None] for _ in range(4)]
        for k in range(2):
            x = 2 * pair + k
            here, totals = sides(level, x, 16, 2)
            for gy in range(4):
                for t in range(2):
                    r = source[t][x, gy] - (
                        diagonal[t][x, gy] * here[gy][t] - 0.125 * totals[gy][t]
                    )
                    sums[gy][t] = r if k == 0 else sums[gy][t] + r
        for gy in range(4):
            for t in range(2):
                r = 0.5 * pair_sum(sums[gy][t], lane, row)
                source_two[t][pair, gy] = scale_two[t][pair, gy] * r

    loop(8, T_REST, residue)

    def sweep_two(old, new):
        def body(x, _):
            here, totals = sides(old, x, 8, 4)
            for gy in range(4):
                for t in range(2):
                    new[t][x, gy] = (
                        (1.0 / 3.0) * here[gy][t]
                        + source_two[t][x, gy]
                        + (0.03125 * scale_two[t][x, gy]) * totals[gy][t]
                    )

        loop(8, T_TWO, body)

    sweep_two(source_two, two_a)
    sweep_two(two_a, two_b)

    def correct(pair, _):
        for k in range(2):
            for gy in range(4):
                for t in range(2):
                    x = 2 * pair + k
                    level[t][x, gy] = level[t][x, gy] + two_b[t][pair, gy]

    loop(8, 4, correct)

    def last(x, _):
        here, totals = sides(level, x, 16, 2, only=1)
        gx, big = x >> 2, x & 3
        for gy in range(4):
            value = (1.0 / 3.0) * here[gy][0] + start_0[x, gy] + scale_0[x, gy] * totals[gy][0]
            out[gx * 4 + gy, pl.ds(pl.multiple_of(big * 8, 8), 8), :] = value

    loop(16, T_LAST, last)


def finish(second, got, out_hbm, out, sems):
    lane, row = lanes(), rows()
    even_lane, even_row = (lane & 1) == 0, (row & 1) == 0

    def group(g, _):
        for big in range(4):
            v = got[g, plane(big), :]
            pair = (
                jnp.where(even_lane, v, lroll(v, 1)),
                jnp.where(even_lane, lroll(v, 127), v),
            )
            for k in range(4):
                w = pair[k % 2]
                if k < 2:
                    w = jnp.where(even_row, w, sroll(w, 1))
                else:
                    w = jnp.where(even_row, sroll(w, 7), w)
                b = g * 4 + k
                for x in (2 * big, 2 * big + 1):
                    out[b, plane(x), :] = second[b, plane(x), :] + w
        return 0

    copies = []
    each = GROUPS // CHUNKS
    for i in range(CHUNKS):
        for g in range(i * each, (i + 1) * each):
            group(g, 0)
        part = pl.ds(i * (BANDS // CHUNKS), BANDS // CHUNKS)
        copies.append(pltpu.make_async_copy(out.at[part], out_hbm.at[part], sems.at[i]))
        copies[i].start()
    for copy in copies:
        copy.wait()


def swap(high, low, axis):
    size = lax.axis_size(axis)
    up = [(i, (i + 1) % size) for i in range(size)]
    return lax.ppermute(high, axis, up), lax.ppermute(low, axis, [(b, a) for a, b in up])


def in_hbm(array):
    return pltpu.with_memory_space_constraint(array, pltpu.HBM)


def local(orbitals, potential, centre, half_width):
    orb = orbitals.reshape(BANDS, 64, 128)
    pot = potential.reshape(64, 128)
    inverse = 1.0 / half_width
    face, wide = shape(BANDS, 8, 128), shape(BANDS + 1, 8, 128)
    thin, block = shape(9, 8, 128), shape(BANDS, 64, 128)

    orb, xhi, xlo, yhi, ylo, zhi, zlo = call(
        pack_fine,
        [HBM, HBM],
        (block, face, face, face, face, thin, thin),
        scratch=(pltpu.VMEM((64, 128), jnp.float32), pltpu.SemaphoreType.DMA((CHUNKS + 1,))),
    )(in_hbm(orb), in_hbm(pot))
    zm, zp = swap(zhi, zlo, "gz")
    ym, yp = swap(yhi, ylo, "gy")
    xm, xp = swap(xhi, xlo, "gx")
    part, by_lane = call(
        first_inside, [SMEM] * 2 + [VMEM] * 2, (block, shape(2, 8, 128)), flops=BUSY
    )(centre, inverse, orb, pot)
    near = (pltpu.VMEM((64, 128), jnp.float32),)
    first, xhi, xlo, yhi, ylo = call(
        first_edges, [SMEM] + [VMEM] * 7, (block, wide, wide, wide, wide), scratch=near
    )(inverse, part, xm, xp, ym, yp, zm, zp)
    ym, yp = swap(yhi, ylo, "gy")
    xm, xp = swap(xhi, xlo, "gx")
    (part,) = call(second_inside, [SMEM] * 2 + [VMEM] * 3, (block,), flops=BUSY)(
        centre, inverse, orb, pot, first
    )
    second, coarse = call(
        second_edges,
        [SMEM] + [VMEM] * 11,
        (block, shape(GROUPS, 40, 128)),
        scratch=near + (pltpu.VMEM((BANDS, 32, 128), jnp.float32),),
        limit=3,
    )(inverse, by_lane, pot, part, xm, xp, ym, yp, zm, zp, zhi, zlo)
    got = lax.all_to_all(coarse, ("gx", "gy"), 0, 0, tiled=True)
    ends = shape(10, 8, 128)
    mhi, mlo = call(pack_ends, [VMEM], (ends, ends))(got)
    left, right = swap(mhi, mlo, "gz")
    lines, half = (16, 4, 8, 128), (8, 4, 8, 128)
    terms = call(
        open_block, [VMEM], (shape(*lines),) * 4 + (shape(*half),), flops=BUSY
    )(got)
    lines, half = pltpu.VMEM(lines, jnp.float32), pltpu.VMEM(half, jnp.float32)
    (level,) = call(
        coarse_solve,
        [VMEM] * 7,
        (shape(GROUPS, 32, 128),),
        scratch=(lines,) * 4 + (half,) + (lines,) * 2 + (half,) * 6,
        limit=6,
    )(left, right, *terms)
    level = lax.all_to_all(level, ("gx", "gy"), 0, 0, tiled=True)
    (out,) = call(
        finish,
        [VMEM] * 2,
        (block,),
        out_specs=(HBM,),
        scratch=(pltpu.VMEM((BANDS, 64, 128), jnp.float32), pltpu.SemaphoreType.DMA((CHUNKS,))),
        limit=4,
    )(second, level)
    return out.reshape(BANDS, 8, 8, 128)


def solution(mesh):
    in_specs = (P(None, "gx", "gy", "gz"), P("gx", "gy", "gz"), P(), P())
    out_specs = P(None, "gx", "gy", "gz")
    return jax.shard_map(local, mesh=mesh, in_specs=in_specs, out_specs=out_specs, check_vma=False)
```

```python
import jax
import jax.numpy as jnp
from jax import lax
from jax.experimental import pallas as pl
from jax.experimental.pallas import tpu as pltpu
from jax.sharding import PartitionSpec as P

BANDS = 64
TILE = (8, 128)
GROUPS = 16
weight = 2.0 / 3.0

VMEM = pl.BlockSpec(memory_space=pltpu.VMEM)
SMEM = pl.BlockSpec(memory_space=pltpu.SMEM)
HBM = pl.BlockSpec(memory_space=pltpu.HBM)
CHUNKS = 4
BUSY = 400_000_000
T_REST_EDGE = 32
T_FIRST, T_INSIDE, T_EDGE, T_SECOND, T_PACK, T_SEND = 16, 16, 32, 32, 16, 8
T_OPEN, T_SWEEP, T_REST, T_TWO, T_LAST = 8, 16, 8, 8, 16


def shape(*dims):
    return jax.ShapeDtypeStruct(dims, jnp.float32)


def call(body, ins, outs, scratch=(), aliases=None, flops=4_000_000, limit=2, out_specs=None):
    return pl.pallas_call(
        body,
        out_shape=outs,
        in_specs=ins,
        out_specs=out_specs or tuple(VMEM for _ in outs),
        scratch_shapes=scratch,
        input_output_aliases=aliases or {},
        compiler_params=pltpu.CompilerParams(vmem_limit_bytes=limit * 1024 * 1024),
        cost_estimate=pl.CostEstimate(flops=flops, bytes_accessed=4_000_000, transcendentals=0),
    )


def lanes():
    return lax.broadcasted_iota(jnp.int32, TILE, 1)


def rows():
    return lax.broadcasted_iota(jnp.int32, TILE, 0)


def lroll(v, shift):
    return pltpu.roll(v, shift, 1)


def sroll(v, shift):
    return pltpu.roll(v, shift, 0)


def plane(x):
    return pl.ds(x * 8, 8)


def loop(count, step, body):
    def several(i, _):
        for k in range(step):
            body(i * step + k, 0)
        return 0

    lax.fori_loop(0, count // step, several, 0)


def nearest(lane, zp, zm, x):
    return jnp.where((lane & 1) == 0, zp[x], zm[x])


def pack_x(orb, pot_hbm, xhi, xlo, pot, sems):
    copies = (
        pltpu.make_async_copy(orb.at[:, plane(7), :], xhi, sems.at[0]),
        pltpu.make_async_copy(orb.at[:, plane(0), :], xlo, sems.at[1]),
        pltpu.make_async_copy(pot_hbm, pot, sems.at[2]),
    )
    for copy in copies:
        copy.start()
    for copy in copies:
        copy.wait()


def pack_yz(orb, pot, yhi, ylo, zhi, zlo):
    lane = lanes()

    def put(carry, v, slot):
        high, low = carry
        turned = lroll(v, (2 * slot + 2) & 127)
        high = jnp.where((lane >> 1) == slot, turned, high)
        low = jnp.where((lane >> 1) == ((slot + 1) & 63), turned, low)
        return high, low

    zero = jnp.zeros(TILE, jnp.float32)

    def body(i, carry):
        carry = list(carry)
        for k in range(T_FIRST):
            b = i * T_FIRST + k
            for x in range(8):
                carry[x] = put(carry[x], orb[b, plane(x), :], b)
            yhi[b] = orb[b, pl.ds(7, 8, stride=8), :]
            ylo[b] = orb[b, pl.ds(0, 8, stride=8), :]
        return tuple(carry)

    carry = lax.fori_loop(0, BANDS // T_FIRST, body, tuple((zero, zero) for _ in range(8)))
    for x in range(8):
        zhi[x] = carry[x][0]
        zlo[x] = lroll(carry[x][1], 126)
    edge = (zero, zero)
    for x in range(8):
        edge = put(edge, pot[plane(x), :], x)
    zhi[8] = edge[0]
    zlo[8] = lroll(edge[1], 126)


def inner_sum(get, x, lane, row):
    v = get(x)
    up = jnp.where(row == 7, 0.0, sroll(v, 7))
    down = jnp.where(row == 0, 0.0, sroll(v, 1))
    ahead = jnp.where(lane == 127, 0.0, lroll(v, 127))
    behind = jnp.where(lane == 0, 0.0, lroll(v, 1))
    total = (up + down) + (ahead + behind)
    if x > 0:
        total = total + get(x - 1)
    if x < 7:
        total = total + get(x + 1)
    return v, total


def outer_sum(x, b, xm, xp, ym, yp, halo, ends, row):
    total = jnp.where(ends, lroll(halo, 127 - 2 * b), 0.0)
    y = jnp.where(row == 0, ym[b, pl.ds(x, 1), :], yp[b, pl.ds(x, 1), :])
    total = total + jnp.where((row == 0) | (row == 7), y, 0.0)
    if x == 0:
        total = total + xm[b]
    if x == 7:
        total = total + xp[b]
    return total


def first_inside(middle, inverse, orb, pot, first, by_lane):
    lane, row = lanes(), rows()
    step = T_INSIDE

    def body(i, carry):
        lane_c, lane_r = carry
        for k in range(step):
            b = i * step + k
            c, r = middle[b], inverse[b]
            lane_c = jnp.where((lane >> 1) == b, c, lane_c)
            lane_r = jnp.where((lane >> 1) == b, r, lane_r)
            get = lambda x: orb[b, plane(x), :]
            for x in range(8):
                v, total = inner_sum(get, x, lane, row)
                first[b, plane(x), :] = (((3.0 - c) + pot[plane(x), :]) * v - 0.5 * total) * r
        return lane_c, lane_r

    zero = jnp.zeros(TILE, jnp.float32)
    by_lane[0], by_lane[1] = lax.fori_loop(0, BANDS // step, body, (zero, zero))


def first_faces(inverse, part, xm, xp, ym, yp, zm, zp, xhi, xlo, yhi, ylo, near):
    lane, row = lanes(), rows()
    ends = (lane == 0) | (lane == 127)
    for x in range(8):
        near[plane(x), :] = nearest(lane, zp, zm, x)

    def body(i, _):
        for k in range(T_EDGE):
            b = i * T_EDGE + k
            r = -0.5 * inverse[b]
            for x, out in ((0, xlo), (7, xhi)):
                total = outer_sum(x, b, xm, xp, ym, yp, near[plane(x), :], ends, row)
                out[b] = part[b, plane(x), :] + r * total
            for y, halo, out in ((0, ym, ylo), (7, yp, yhi)):
                cells = pl.ds(y, 8, stride=8)
                total = halo[b] + jnp.where(ends, lroll(near[cells, :], 127 - 2 * b), 0.0)
                side = jnp.where(row == 0, xm[b, pl.ds(y, 1), :], xp[b, pl.ds(y, 1), :])
                total = total + jnp.where((row == 0) | (row == 7), side, 0.0)
                out[b] = part[b, cells, :] + r * total
        return 0

    lax.fori_loop(0, BANDS // T_EDGE, body, 0)
    xhi[BANDS] = near[plane(7), :]
    xlo[BANDS] = near[plane(0), :]
    yhi[BANDS] = near[pl.ds(7, 8, stride=8), :]
    ylo[BANDS] = near[pl.ds(0, 8, stride=8), :]


def first_edges(inverse, part, xm, xp, ym, yp, zm, zp, first, near):
    lane, row = lanes(), rows()
    ends = (lane == 0) | (lane == 127)
    for x in range(8):
        near[plane(x), :] = nearest(lane, zp, zm, x)

    def body(i, _):
        for k in range(T_REST_EDGE):
            b = i * T_REST_EDGE + k
            r = -0.5 * inverse[b]
            for x in range(8):
                total = outer_sum(x, b, xm, xp, ym, yp, near[plane(x), :], ends, row)
                first[b, plane(x), :] = part[b, plane(x), :] + r * total
        return 0

    lax.fori_loop(0, BANDS // T_REST_EDGE, body, 0)


def second_inside(middle, inverse, orb, pot, first, second):
    lane, row = lanes(), rows()
    step = T_INSIDE

    def body(i, _):
        for k in range(step):
            b = i * step + k
            c, r = middle[b], 2.0 * inverse[b]
            get = lambda x: first[b, plane(x), :]
            for x in range(8):
                v, total = inner_sum(get, x, lane, row)
                value = (((3.0 - c) + pot[plane(x), :]) * v - 0.5 * total) * r
                second[b, plane(x), :] = value - orb[b, plane(x), :]
        return 0

    lax.fori_loop(0, BANDS // step, body, 0)


def second_edges(
    inverse, by_lane, pot, part, xm, xp, ym, yp, zm, zp, zhi, zlo,
    second, coarse, edge, sums,
):
    lane, row = lanes(), rows()
    ends = (lane == 0) | (lane == 127)
    even_lane, even_row = (lane & 1) == 0, (row & 1) == 0

    cells = [nearest(lane, zp, zm, x) for x in range(8)]
    pots = nearest(lane, zp, zm, 8)
    for x in range(8):
        v = cells[x]
        outer = jnp.where(even_lane, lroll(zp[x], 127), lroll(zm[x], 1))
        inner = jnp.where(even_lane, lroll(zhi[x], 127), lroll(zlo[x], 1))
        left = cells[x - 1] if x > 0 else xm[BANDS]
        right = cells[x + 1] if x < 7 else xp[BANDS]
        up = jnp.where(row == 7, yp[BANDS, pl.ds(x, 1), :], sroll(v, 7))
        down = jnp.where(row == 0, ym[BANDS, pl.ds(x, 1), :], sroll(v, 1))
        total = (left + right) + (up + down) + (outer + inner)
        here = jnp.where(even_lane, pots[:, 2 * x : 2 * x + 1], pots[:, 2 * x + 1 : 2 * x + 2])
        edge[plane(x), :] = ((3.0 - by_lane[0] + here) * v - 0.5 * total) * by_lane[1]

    def image(i, _):
        for k in range(T_SECOND):
            b = i * T_SECOND + k
            r = inverse[b]
            for big in range(4):
                pair = []
                for x in (2 * big, 2 * big + 1):
                    total = outer_sum(x, b, xm, xp, ym, yp, edge[plane(x), :], ends, row)
                    pair.append(part[b, plane(x), :] - r * total)
                    second[b, plane(x), :] = pair[-1]
                sums[b, plane(big), :] = pair[0] + pair[1]
        return 0

    def pair_lanes(a, b):
        return jnp.where(even_lane, a + lroll(a, 127), b + lroll(b, 1))

    def pair_rows(a, b):
        return jnp.where(even_row, a + sroll(a, 7), b + sroll(b, 1))

    def pack(g, _):
        for big in range(4):
            v = [sums[g * 4 + k, plane(big), :] for k in range(4)]
            coarse[g, plane(big), :] = 0.5 * pair_rows(pair_lanes(v[0], v[1]), pair_lanes(v[2], v[3]))

    four = [pot[plane(2 * i), :] + pot[plane(2 * i + 1), :] for i in range(4)]
    packed = 0.125 * pair_rows(pair_lanes(four[0], four[1]), pair_lanes(four[2], four[3]))
    for g in range(GROUPS):
        coarse[g, plane(4), :] = packed
    lax.fori_loop(0, BANDS // T_SECOND, image, 0)
    loop(GROUPS, T_PACK, pack)


def pack_ends(got, mhi, mlo):
    lane = lanes()
    zero = jnp.zeros(TILE, jnp.float32)

    def send(half, _):
        high = low = zero
        for odd in range(2):
            for big in range(4):
                v = got[2 * half + odd, plane(big), :]
                mine = (lane >> 4) == 2 * big + odd
                at = 32 * big + 16 * odd
                high = jnp.where(mine, lroll(v, (at + 16) & 127), high)
                low = jnp.where(mine, lroll(v, at), low)
        mhi[half] = high
        mlo[half] = low

    loop(GROUPS // 2, T_SEND, send)
    for half in range(2):
        high = low = zero
        for i in range(8):
            v = got[8 * half + i, plane(4), :]
            high = jnp.where((lane >> 4) == i, lroll(v, (16 * i + 16) & 127), high)
            low = jnp.where((lane >> 4) == i, lroll(v, 16 * i), low)
        mhi[8 + half] = high
        mlo[8 + half] = low


def coarse_terms(blocks, pots, gx, gy, source, diagonal, scale, start, scale_two):
    lane, row = lanes(), rows()
    even_lane, even_row = (lane & 1) == 0, (row & 1) == 0
    a = jnp.where(even_lane, pots, lroll(pots, 1))
    b = jnp.where(even_lane, lroll(pots, 127), pots)
    each = []
    for up in (False, True):
        for w in (a, b):
            each.append(jnp.where(even_row, sroll(w, 7), w) if up else jnp.where(even_row, w, sroll(w, 1)))
    for big in range(4):
        at = (gx * 4 + big, gy)
        d = each[big] + 0.8
        w = weight / d
        source[at] = blocks[big]
        diagonal[at] = d
        scale[at] = 0.125 * w
        start[at] = w * blocks[big]
    for k in range(2):
        p = 0.125 * pair_sum(each[2 * k] + each[2 * k + 1], lane, row)
        scale_two[gx * 2 + k, gy] = weight / (p + 0.2375)


def pair_sum(v, lane, row):
    v = v + jnp.where((row & 2) == 0, sroll(v, 6), sroll(v, 2))
    return v + jnp.where((lane & 2) == 0, lroll(v, 126), lroll(v, 2))


def open_block(got, source, diagonal, scale, start, scale_two):
    def unpack(src, _):
        blocks = [got[src, plane(big), :] for big in range(4)]
        pots = got[src, plane(4), :]
        coarse_terms(blocks, pots, src >> 2, src & 3, source, diagonal, scale, start, scale_two)

    loop(GROUPS, T_OPEN, unpack)


def coarse_solve(
    left, right, source_0, diagonal_0, scale_0, start_0, scale_two_0, out,
    source_1, diagonal_1, scale_1, start_1, scale_two_1,
    level_0, level_1, source_two_0, source_two_1, two_0, two_1,
):
    lane, row = lanes(), rows()
    source, diagonal = (source_0, source_1), (diagonal_0, diagonal_1)
    scale, start = (scale_0, scale_1), (start_0, start_1)
    scale_two, level = (scale_two_0, scale_two_1), (level_0, level_1)
    source_two, two = (source_two_0, source_two_1), (two_0, two_1)

    def unpack(group, _):
        for i in range(8):
            src = 8 * group + i
            a, b = left[4 * group + i // 2], right[4 * group + i // 2]
            if i % 2 == 0:
                b = lroll(b, 16)
            else:
                a = lroll(a, 112)
            halo = jnp.where(((lane >> 4) & 1) == 0, a, b)
            blocks = [lroll(halo, 112 - 32 * big) for big in range(4)]
            near, far = right[8 + group], left[8 + group]
            pots = jnp.where(lane < 64, lroll(near, (128 - 16 * i) & 127), lroll(far, 112 - 16 * i))
            coarse_terms(
                blocks, pots, 2 * group + i // 4, i % 4,
                source_1, diagonal_1, scale_1, start_1, scale_two_1,
            )

    loop(2, 1, unpack)

    def load(ref, x):
        return [[ref[t][x, gy] for t in range(2)] for gy in range(4)]

    def sides(ref, x, count, step, only=2):
        here = load(ref, x)
        before = lax.rem(x + (count - 1), count)
        after = lax.rem(x + 1, count)
        down = [[sroll(here[gy][t], step) for t in range(2)] for gy in range(4)]
        up = [[sroll(here[gy][t], 8 - step) for t in range(2)] for gy in range(4)] if step != 4 else down
        behind = [[lroll(here[gy][t], step) for t in range(2)] for gy in range(4)]
        ahead = [[lroll(here[gy][t], 128 - step) for t in range(2)] for gy in range(4)]
        totals = []
        for gy in range(4):
            line = []
            for t in range(only):
                total = ref[t][before, gy] + ref[t][after, gy]
                y = jnp.where(row < step, down[(gy + 3) % 4][t], down[gy][t])
                y = y + jnp.where(row >= 8 - step, up[(gy + 1) % 4][t], up[gy][t])
                z = jnp.where(lane < step, behind[gy][1 - t], behind[gy][t])
                z = z + jnp.where(lane >= 128 - step, ahead[gy][1 - t], ahead[gy][t])
                line.append(total + y + z)
            totals.append(line)
        return here, totals

    def sweep_one(x, _):
        here, totals = sides(start, x, 16, 2)
        for gy in range(4):
            for t in range(2):
                value = (4.0 / 3.0) * here[gy][t] + scale[t][x, gy] * totals[gy][t]
                level[t][x, gy] = value

    loop(16, T_SWEEP, sweep_one)

    def residue(pair, _):
        sums = [[None, None] for _ in range(4)]
        for k in range(2):
            x = 2 * pair + k
            here, totals = sides(level, x, 16, 2)
            for gy in range(4):
                for t in range(2):
                    r = source[t][x, gy] - (
                        diagonal[t][x, gy] * here[gy][t] - 0.125 * totals[gy][t]
                    )
                    sums[gy][t] = r if k == 0 else sums[gy][t] + r
        for gy in range(4):
            for t in range(2):
                r = 0.5 * pair_sum(sums[gy][t], lane, row)
                source_two[t][pair, gy] = scale_two[t][pair, gy] * r

    loop(8, T_REST, residue)

    def sweep_two(old, write):
        def body(x, _):
            here, totals = sides(old, x, 8, 4)
            for gy in range(4):
                for t in range(2):
                    value = (
                        (1.0 / 3.0) * here[gy][t]
                        + source_two[t][x, gy]
                        + (0.03125 * scale_two[t][x, gy]) * totals[gy][t]
                    )
                    write(x, gy, t, value)

        loop(8, T_TWO, body)

    def keep(x, gy, t, value):
        two[t][x, gy] = value

    def correct(pair, gy, t, value):
        for x in (2 * pair, 2 * pair + 1):
            level[t][x, gy] = level[t][x, gy] + value

    sweep_two(source_two, keep)
    sweep_two(two, correct)

    def last(x, _):
        here, totals = sides(level, x, 16, 2, only=1)
        gx, big = x >> 2, x & 3
        for gy in range(4):
            value = (1.0 / 3.0) * here[gy][0] + start_0[x, gy] + scale_0[x, gy] * totals[gy][0]
            out[gx * 4 + gy, pl.ds(pl.multiple_of(big * 8, 8), 8), :] = value

    loop(16, T_LAST, last)


def finish(second, got, out_hbm, out, sems):
    lane, row = lanes(), rows()
    even_lane, even_row = (lane & 1) == 0, (row & 1) == 0

    def group(g, _):
        for big in range(4):
            v = got[g, plane(big), :]
            pair = (
                jnp.where(even_lane, v, lroll(v, 1)),
                jnp.where(even_lane, lroll(v, 127), v),
            )
            for k in range(4):
                w = pair[k % 2]
                if k < 2:
                    w = jnp.where(even_row, w, sroll(w, 1))
                else:
                    w = jnp.where(even_row, sroll(w, 7), w)
                b = g * 4 + k
                for x in (2 * big, 2 * big + 1):
                    out[b, plane(x), :] = second[b, plane(x), :] + w
        return 0

    copies = []
    each = GROUPS // CHUNKS
    for i in range(CHUNKS):
        for g in range(i * each, (i + 1) * each):
            group(g, 0)
        part = pl.ds(i * (BANDS // CHUNKS), BANDS // CHUNKS)
        copies.append(pltpu.make_async_copy(out.at[part], out_hbm.at[part], sems.at[i]))
        copies[i].start()
    for copy in copies:
        copy.wait()


def swap(high, low, axis):
    size = lax.axis_size(axis)
    up = [(i, (i + 1) % size) for i in range(size)]
    return lax.ppermute(high, axis, up), lax.ppermute(low, axis, [(b, a) for a, b in up])


def in_hbm(array):
    return pltpu.with_memory_space_constraint(array, pltpu.HBM)


def local(orbitals, potential, centre, half_width):
    orb = orbitals.reshape(BANDS, 64, 128)
    pot = potential.reshape(64, 128)
    inverse = 1.0 / half_width
    face, wide = shape(BANDS, 8, 128), shape(BANDS + 1, 8, 128)
    thin, block = shape(9, 8, 128), shape(BANDS, 64, 128)

    xhi, xlo, pot = call(
        pack_x,
        [HBM] * 2,
        (face, face, shape(64, 128)),
        scratch=(pltpu.SemaphoreType.DMA((3,)),),
    )(in_hbm(orb), in_hbm(pot))
    yhi, ylo, zhi, zlo = call(pack_yz, [VMEM] * 2, (face, face, thin, thin))(orb, pot)
    zm, zp = swap(zhi, zlo, "gz")
    ym, yp = swap(yhi, ylo, "gy")
    xm, xp = swap(xhi, xlo, "gx")
    part, by_lane = call(
        first_inside, [SMEM] * 2 + [VMEM] * 2, (block, shape(2, 8, 128)), flops=BUSY
    )(centre, inverse, orb, pot)
    near = (pltpu.VMEM((64, 128), jnp.float32),)
    halos = (inverse, part, xm, xp, ym, yp, zm, zp)
    xhi, xlo, yhi, ylo = call(first_faces, [SMEM] + [VMEM] * 7, (wide,) * 4, scratch=near)(*halos)
    (first,) = call(first_edges, [SMEM] + [VMEM] * 7, (block,), scratch=near, flops=BUSY)(*halos)
    ym, yp = swap(yhi, ylo, "gy")
    xm, xp = swap(xhi, xlo, "gx")
    (part,) = call(second_inside, [SMEM] * 2 + [VMEM] * 3, (block,), flops=BUSY)(
        centre, inverse, orb, pot, first
    )
    second, coarse = call(
        second_edges,
        [SMEM] + [VMEM] * 11,
        (block, shape(GROUPS, 40, 128)),
        scratch=near + (pltpu.VMEM((BANDS, 32, 128), jnp.float32),),
        limit=3,
    )(inverse, by_lane, pot, part, xm, xp, ym, yp, zm, zp, zhi, zlo)
    got = lax.all_to_all(coarse, ("gx", "gy"), 0, 0, tiled=True)
    ends = shape(10, 8, 128)
    mhi, mlo = call(pack_ends, [VMEM], (ends, ends))(got)
    left, right = swap(mhi, mlo, "gz")
    lines, half = (16, 4, 8, 128), (8, 4, 8, 128)
    terms = call(
        open_block, [VMEM], (shape(*lines),) * 4 + (shape(*half),), flops=BUSY
    )(got)
    lines, half = pltpu.VMEM(lines, jnp.float32), pltpu.VMEM(half, jnp.float32)
    (level,) = call(
        coarse_solve,
        [VMEM] * 7,
        (shape(GROUPS, 32, 128),),
        scratch=(lines,) * 4 + (half,) + (lines,) * 2 + (half,) * 4,
        limit=6,
    )(left, right, *terms)
    level = lax.all_to_all(level, ("gx", "gy"), 0, 0, tiled=True)
    (out,) = call(
        finish,
        [VMEM] * 2,
        (block,),
        out_specs=(HBM,),
        scratch=(pltpu.VMEM((BANDS, 64, 128), jnp.float32), pltpu.SemaphoreType.DMA((CHUNKS,))),
        limit=4,
    )(second, level)
    return out.reshape(BANDS, 8, 8, 128)


def solution(mesh):
    in_specs = (P(None, "gx", "gy", "gz"), P("gx", "gy", "gz"), P(), P())
    out_specs = P(None, "gx", "gy", "gz")
    return jax.shard_map(local, mesh=mesh, in_specs=in_specs, out_specs=out_specs, check_vma=False)
```

```python
import jax
import jax.numpy as jnp
from jax import lax
from jax.experimental import pallas as pl
from jax.experimental.pallas import tpu as pltpu
from jax.sharding import PartitionSpec as P

BANDS = 64
TILE = (8, 128)
GROUPS = 16
weight = 2.0 / 3.0

VMEM = pl.BlockSpec(memory_space=pltpu.VMEM)
SMEM = pl.BlockSpec(memory_space=pltpu.SMEM)
HBM = pl.BlockSpec(memory_space=pltpu.HBM)
CHUNKS = 4
BUSY = 400_000_000
T_REST_EDGE = 32
T_FIRST, T_INSIDE, T_EDGE, T_SECOND, T_PACK, T_SEND = 32, 16, 64, 16, 16, 8
T_OPEN, T_SWEEP, T_REST, T_TWO, T_LAST = 8, 16, 8, 8, 16


def shape(*dims):
    return jax.ShapeDtypeStruct(dims, jnp.float32)


def call(body, ins, outs, scratch=(), aliases=None, flops=4_000_000, limit=2, out_specs=None):
    return pl.pallas_call(
        body,
        out_shape=outs,
        in_specs=ins,
        out_specs=out_specs or tuple(VMEM for _ in outs),
        scratch_shapes=scratch,
        input_output_aliases=aliases or {},
        compiler_params=pltpu.CompilerParams(vmem_limit_bytes=limit * 1024 * 1024),
        cost_estimate=pl.CostEstimate(flops=flops, bytes_accessed=4_000_000, transcendentals=0),
    )


def lanes():
    return lax.broadcasted_iota(jnp.int32, TILE, 1)


def rows():
    return lax.broadcasted_iota(jnp.int32, TILE, 0)


def lroll(v, shift):
    return pltpu.roll(v, shift, 1)


def sroll(v, shift):
    return pltpu.roll(v, shift, 0)


def plane(x):
    return pl.ds(x * 8, 8)


def loop(count, step, body):
    def several(i, _):
        for k in range(step):
            body(i * step + k, 0)
        return 0

    lax.fori_loop(0, count // step, several, 0)


def nearest(lane, zp, zm, x):
    return jnp.where((lane & 1) == 0, zp[x], zm[x])


def pack_x(orb, pot_hbm, xhi, xlo, pot, sems):
    copies = (
        pltpu.make_async_copy(orb.at[:, plane(7), :], xhi, sems.at[0]),
        pltpu.make_async_copy(orb.at[:, plane(0), :], xlo, sems.at[1]),
        pltpu.make_async_copy(pot_hbm, pot, sems.at[2]),
    )
    for copy in copies:
        copy.start()
    for copy in copies:
        copy.wait()


def pack_yz(orb, pot, yhi, ylo, zhi, zlo):
    lane = lanes()

    def put(carry, v, slot):
        high, low = carry
        turned = lroll(v, (2 * slot + 2) & 127)
        high = jnp.where((lane >> 1) == slot, turned, high)
        low = jnp.where((lane >> 1) == ((slot + 1) & 63), turned, low)
        return high, low

    zero = jnp.zeros(TILE, jnp.float32)

    def body(i, carry):
        carry = list(carry)
        for k in range(T_FIRST):
            b = i * T_FIRST + k
            for x in range(8):
                carry[x] = put(carry[x], orb[b, plane(x), :], b)
            yhi[b] = orb[b, pl.ds(7, 8, stride=8), :]
            ylo[b] = orb[b, pl.ds(0, 8, stride=8), :]
        return tuple(carry)

    carry = lax.fori_loop(0, BANDS // T_FIRST, body, tuple((zero, zero) for _ in range(8)))
    for x in range(8):
        zhi[x] = carry[x][0]
        zlo[x] = lroll(carry[x][1], 126)
    edge = (zero, zero)
    for x in range(8):
        edge = put(edge, pot[plane(x), :], x)
    zhi[8] = edge[0]
    zlo[8] = lroll(edge[1], 126)


def inner_sum(get, x, lane, row):
    v = get(x)
    up = jnp.where(row == 7, 0.0, sroll(v, 7))
    down = jnp.where(row == 0, 0.0, sroll(v, 1))
    ahead = jnp.where(lane == 127, 0.0, lroll(v, 127))
    behind = jnp.where(lane == 0, 0.0, lroll(v, 1))
    total = (up + down) + (ahead + behind)
    if x > 0:
        total = total + get(x - 1)
    if x < 7:
        total = total + get(x + 1)
    return v, total


def outer_sum(x, b, xm, xp, ym, yp, halo, ends, row):
    total = jnp.where(ends, lroll(halo, 127 - 2 * b), 0.0)
    y = jnp.where(row == 0, ym[b, pl.ds(x, 1), :], yp[b, pl.ds(x, 1), :])
    total = total + jnp.where((row == 0) | (row == 7), y, 0.0)
    if x == 0:
        total = total + xm[b]
    if x == 7:
        total = total + xp[b]
    return total


def first_inside(middle, inverse, orb, pot, first, by_lane):
    lane, row = lanes(), rows()
    step = T_INSIDE

    def body(i, carry):
        lane_c, lane_r = carry
        for k in range(step):
            b = i * step + k
            c, r = middle[b], inverse[b]
            lane_c = jnp.where((lane >> 1) == b, c, lane_c)
            lane_r = jnp.where((lane >> 1) == b, r, lane_r)
            get = lambda x: orb[b, plane(x), :]
            for x in range(8):
                v, total = inner_sum(get, x, lane, row)
                first[b, plane(x), :] = (((3.0 - c) + pot[plane(x), :]) * v - 0.5 * total) * r
        return lane_c, lane_r

    zero = jnp.zeros(TILE, jnp.float32)
    by_lane[0], by_lane[1] = lax.fori_loop(0, BANDS // step, body, (zero, zero))


def pack_four(v, lane, row):
    even_lane, even_row = (lane & 1) == 0, (row & 1) == 0
    a = jnp.where(even_lane, v[0] + lroll(v[0], 127), v[1] + lroll(v[1], 1))
    b = jnp.where(even_lane, v[2] + lroll(v[2], 127), v[3] + lroll(v[3], 1))
    return jnp.where(even_row, a + sroll(a, 7), b + sroll(b, 1))


def first_faces(
    inverse, part, xm, xp, ym, yp, zm, zp, xhi, xlo, yhi, ylo, cxhi, cxlo, cyhi, cylo, near
):
    lane, row = lanes(), rows()
    ends = (lane == 0) | (lane == 127)
    for x in range(8):
        near[plane(x), :] = nearest(lane, zp, zm, x)

    def body(i, _):
        for k in range(T_EDGE):
            b = i * T_EDGE + k
            r = -0.5 * inverse[b]
            for x, out in ((0, xlo), (7, xhi)):
                total = outer_sum(x, b, xm, xp, ym, yp, near[plane(x), :], ends, row)
                out[b] = part[b, plane(x), :] + r * total
            for y, halo, out in ((0, ym, ylo), (7, yp, yhi)):
                cells = pl.ds(y, 8, stride=8)
                total = halo[b] + jnp.where(ends, lroll(near[cells, :], 127 - 2 * b), 0.0)
                side = jnp.where(row == 0, xm[b, pl.ds(y, 1), :], xp[b, pl.ds(y, 1), :])
                total = total + jnp.where((row == 0) | (row == 7), side, 0.0)
                out[b] = part[b, cells, :] + r * total
        return 0

    lax.fori_loop(0, BANDS // T_EDGE, body, 0)

    def coarsen(g, _):
        for face, out in ((xhi, cxhi), (xlo, cxlo), (yhi, cyhi), (ylo, cylo)):
            out[g] = pack_four([face[g * 4 + k] for k in range(4)], lane, row)

    loop(GROUPS, T_PACK, coarsen)
    cxhi[GROUPS] = near[plane(7), :]
    cxlo[GROUPS] = near[plane(0), :]
    cyhi[GROUPS] = near[pl.ds(7, 8, stride=8), :]
    cylo[GROUPS] = near[pl.ds(0, 8, stride=8), :]


def first_edges(inverse, part, xm, xp, ym, yp, zm, zp, first, near):
    lane, row = lanes(), rows()
    ends = (lane == 0) | (lane == 127)
    for x in range(8):
        near[plane(x), :] = nearest(lane, zp, zm, x)

    def body(i, _):
        for k in range(T_REST_EDGE):
            b = i * T_REST_EDGE + k
            r = -0.5 * inverse[b]
            for x in range(8):
                total = outer_sum(x, b, xm, xp, ym, yp, near[plane(x), :], ends, row)
                first[b, plane(x), :] = part[b, plane(x), :] + r * total
        return 0

    lax.fori_loop(0, BANDS // T_REST_EDGE, body, 0)


def chunk(i):
    return pl.ds(i * (BANDS // CHUNKS), BANDS // CHUNKS)


def second_inside(middle, inverse, orb, pot, first, second_hbm, packed, second, sems):
    lane, row = lanes(), rows()
    step = T_INSIDE

    def body(i, _):
        for k in range(step):
            b = i * step + k
            c, r = middle[b], 2.0 * inverse[b]
            get = lambda x: first[b, plane(x), :]
            for x in range(8):
                v, total = inner_sum(get, x, lane, row)
                value = (((3.0 - c) + pot[plane(x), :]) * v - 0.5 * total) * r
                second[b, plane(x), :] = value - orb[b, plane(x), :]
        return 0

    copies = []
    each = BANDS // CHUNKS // step
    for i in range(CHUNKS):
        lax.fori_loop(i * each, (i + 1) * each, body, 0)
        copies.append(pltpu.make_async_copy(second.at[chunk(i)], second_hbm.at[chunk(i)], sems.at[i]))
        copies[i].start()

    def coarsen(g, _):
        for big in range(4):
            low, high = plane(2 * big), plane(2 * big + 1)
            v = [second[g * 4 + k, low, :] + second[g * 4 + k, high, :] for k in range(4)]
            packed[g, plane(big), :] = 0.5 * pack_four(v, lane, row)

    loop(GROUPS, 8, coarsen)
    four = [pot[plane(2 * i), :] + pot[plane(2 * i + 1), :] for i in range(4)]
    pots = 0.125 * pack_four(four, lane, row)
    for g in range(GROUPS):
        packed[g, plane(4), :] = pots
    for copy in copies:
        copy.wait()


def coarse_edges(
    inverse, by_lane, pot, packed, xm, xp, ym, yp, zm, zp, zhi, zlo, face_0, face_1, face_2, face_3,
    coarse_hbm, edge, same_0, same_1, same_2, same_3, coarse, sems,
):
    lane, row = lanes(), rows()
    even_lane, even_row = (lane & 1) == 0, (row & 1) == 0

    cells = [nearest(lane, zp, zm, x) for x in range(8)]
    pots = nearest(lane, zp, zm, 8)
    values = []
    for x in range(8):
        v = cells[x]
        outer = jnp.where(even_lane, lroll(zp[x], 127), lroll(zm[x], 1))
        inner = jnp.where(even_lane, lroll(zhi[x], 127), lroll(zlo[x], 1))
        left = cells[x - 1] if x > 0 else xm[GROUPS]
        right = cells[x + 1] if x < 7 else xp[GROUPS]
        up = jnp.where(row == 7, yp[GROUPS, pl.ds(x, 1), :], sroll(v, 7))
        down = jnp.where(row == 0, ym[GROUPS, pl.ds(x, 1), :], sroll(v, 1))
        total = (left + right) + (up + down) + (outer + inner)
        here = jnp.where(even_lane, pots[:, 2 * x : 2 * x + 1], pots[:, 2 * x + 1 : 2 * x + 2])
        values.append(((3.0 - by_lane[0] + here) * v - 0.5 * total) * by_lane[1])
        edge[plane(x), :] = values[x]

    ends = []
    for big in range(4):
        v = values[2 * big] + values[2 * big + 1]
        v = v + jnp.where(even_row, sroll(v, 7), sroll(v, 1))
        place = lane & 3
        ends.append(jnp.where(place == 1, lroll(v, 127), jnp.where(place == 2, lroll(v, 1), v)))
    outside = (lane < 2) | (lane >= 126)

    def group(g, _):
        r = [inverse[g * 4 + k] for k in range(4)]
        half = -0.5 * jnp.where(
            even_row, jnp.where(even_lane, r[0], r[1]), jnp.where(even_lane, r[2], r[3])
        )
        for big in range(4):
            z = jnp.where(
                even_row,
                lroll(ends[big], (254 - 8 * g) & 127),
                lroll(ends[big], (250 - 8 * g) & 127),
            )
            y = jnp.where(row < 2, sroll(ym[g], (8 - 2 * big) % 8), sroll(yp[g], 6 - 2 * big))
            total = jnp.where(outside, z, 0.0) + jnp.where((row < 2) | (row >= 6), y, 0.0)
            if big == 0:
                total = total + xm[g]
            if big == 3:
                total = total + xp[g]
            coarse[g, plane(big), :] = packed[g, plane(big), :] + half * total
        coarse[g, plane(4), :] = packed[g, plane(4), :]

    copies = []
    for i in range(2):
        for g in range(8 * i, 8 * i + 8):
            group(g, 0)
        half = pl.ds(8 * i, 8)
        copies.append(pltpu.make_async_copy(coarse.at[half], coarse_hbm.at[half], sems.at[i]))
        copies[i].start()
    for copy in copies:
        copy.wait()


def second_edges(inverse, part_hbm, xm, xp, ym, yp, edge, second, part, sems):
    lane, row = lanes(), rows()
    ends = (lane == 0) | (lane == 127)
    copies = []
    for i in range(CHUNKS):
        copies.append(pltpu.make_async_copy(part_hbm.at[chunk(i)], part.at[chunk(i)], sems.at[i]))
        copies[i].start()

    def body(i, _):
        for k in range(T_SECOND):
            b = i * T_SECOND + k
            r = inverse[b]
            for x in range(8):
                total = outer_sum(x, b, xm, xp, ym, yp, edge[plane(x), :], ends, row)
                second[b, plane(x), :] = part[b, plane(x), :] - r * total
        return 0

    each = BANDS // CHUNKS // T_SECOND
    for i in range(CHUNKS):
        copies[i].wait()
        lax.fori_loop(i * each, (i + 1) * each, body, 0)


def pack_ends(got, mhi, mlo):
    lane = lanes()
    zero = jnp.zeros(TILE, jnp.float32)

    def send(half, _):
        high = low = zero
        for odd in range(2):
            for big in range(4):
                v = got[2 * half + odd, plane(big), :]
                mine = (lane >> 4) == 2 * big + odd
                at = 32 * big + 16 * odd
                high = jnp.where(mine, lroll(v, (at + 16) & 127), high)
                low = jnp.where(mine, lroll(v, at), low)
        mhi[half] = high
        mlo[half] = low

    loop(GROUPS // 2, T_SEND, send)
    for half in range(2):
        high = low = zero
        for i in range(8):
            v = got[8 * half + i, plane(4), :]
            high = jnp.where((lane >> 4) == i, lroll(v, (16 * i + 16) & 127), high)
            low = jnp.where((lane >> 4) == i, lroll(v, 16 * i), low)
        mhi[8 + half] = high
        mlo[8 + half] = low


def coarse_terms(blocks, pots, gx, gy, source, diagonal, scale, start, scale_two):
    lane, row = lanes(), rows()
    even_lane, even_row = (lane & 1) == 0, (row & 1) == 0
    a = jnp.where(even_lane, pots, lroll(pots, 1))
    b = jnp.where(even_lane, lroll(pots, 127), pots)
    each = []
    for up in (False, True):
        for w in (a, b):
            each.append(jnp.where(even_row, sroll(w, 7), w) if up else jnp.where(even_row, w, sroll(w, 1)))
    for big in range(4):
        at = (gx * 4 + big, gy)
        d = each[big] + 0.8
        w = weight / d
        source[at] = blocks[big]
        diagonal[at] = d
        scale[at] = 0.125 * w
        start[at] = w * blocks[big]
    for k in range(2):
        p = 0.125 * pair_sum(each[2 * k] + each[2 * k + 1], lane, row)
        scale_two[gx * 2 + k, gy] = weight / (p + 0.2375)


def pair_sum(v, lane, row):
    v = v + jnp.where((row & 2) == 0, sroll(v, 6), sroll(v, 2))
    return v + jnp.where((lane & 2) == 0, lroll(v, 126), lroll(v, 2))


def open_block(got, source, diagonal, scale, start, scale_two):
    def unpack(src, _):
        blocks = [got[src, plane(big), :] for big in range(4)]
        pots = got[src, plane(4), :]
        coarse_terms(blocks, pots, src >> 2, src & 3, source, diagonal, scale, start, scale_two)

    loop(GROUPS, T_OPEN, unpack)


def coarse_solve(
    left, right, source_0, diagonal_0, scale_0, start_0, scale_two_0, second, out,
    source_1, diagonal_1, scale_1, start_1, scale_two_1,
    level_0, level_1, source_two_0, source_two_1, two_0, two_1,
):
    lane, row = lanes(), rows()
    source, diagonal = (source_0, source_1), (diagonal_0, diagonal_1)
    scale, start = (scale_0, scale_1), (start_0, start_1)
    scale_two, level = (scale_two_0, scale_two_1), (level_0, level_1)
    source_two, two = (source_two_0, source_two_1), (two_0, two_1)

    def unpack(group, _):
        for i in range(8):
            src = 8 * group + i
            a, b = left[4 * group + i // 2], right[4 * group + i // 2]
            if i % 2 == 0:
                b = lroll(b, 16)
            else:
                a = lroll(a, 112)
            halo = jnp.where(((lane >> 4) & 1) == 0, a, b)
            blocks = [lroll(halo, 112 - 32 * big) for big in range(4)]
            near, far = right[8 + group], left[8 + group]
            pots = jnp.where(lane < 64, lroll(near, (128 - 16 * i) & 127), lroll(far, 112 - 16 * i))
            coarse_terms(
                blocks, pots, 2 * group + i // 4, i % 4,
                source_1, diagonal_1, scale_1, start_1, scale_two_1,
            )

    loop(2, 1, unpack)

    def load(ref, x):
        return [[ref[t][x, gy] for t in range(2)] for gy in range(4)]

    def sides(ref, x, count, step, only=2):
        here = load(ref, x)
        before = lax.rem(x + (count - 1), count)
        after = lax.rem(x + 1, count)
        down = [[sroll(here[gy][t], step) for t in range(2)] for gy in range(4)]
        up = [[sroll(here[gy][t], 8 - step) for t in range(2)] for gy in range(4)] if step != 4 else down
        behind = [[lroll(here[gy][t], step) for t in range(2)] for gy in range(4)]
        ahead = [[lroll(here[gy][t], 128 - step) for t in range(2)] for gy in range(4)]
        totals = []
        for gy in range(4):
            line = []
            for t in range(only):
                total = ref[t][before, gy] + ref[t][after, gy]
                y = jnp.where(row < step, down[(gy + 3) % 4][t], down[gy][t])
                y = y + jnp.where(row >= 8 - step, up[(gy + 1) % 4][t], up[gy][t])
                z = jnp.where(lane < step, behind[gy][1 - t], behind[gy][t])
                z = z + jnp.where(lane >= 128 - step, ahead[gy][1 - t], ahead[gy][t])
                line.append(total + y + z)
            totals.append(line)
        return here, totals

    def sweep_one(x, _):
        here, totals = sides(start, x, 16, 2)
        for gy in range(4):
            for t in range(2):
                value = (4.0 / 3.0) * here[gy][t] + scale[t][x, gy] * totals[gy][t]
                level[t][x, gy] = value

    loop(16, T_SWEEP, sweep_one)

    def residue(pair, _):
        sums = [[None, None] for _ in range(4)]
        for k in range(2):
            x = 2 * pair + k
            here, totals = sides(level, x, 16, 2)
            for gy in range(4):
                for t in range(2):
                    r = source[t][x, gy] - (
                        diagonal[t][x, gy] * here[gy][t] - 0.125 * totals[gy][t]
                    )
                    sums[gy][t] = r if k == 0 else sums[gy][t] + r
        for gy in range(4):
            for t in range(2):
                r = 0.5 * pair_sum(sums[gy][t], lane, row)
                source_two[t][pair, gy] = scale_two[t][pair, gy] * r

    loop(8, T_REST, residue)

    def sweep_two(old, write):
        def body(x, _):
            here, totals = sides(old, x, 8, 4)
            for gy in range(4):
                for t in range(2):
                    value = (
                        (1.0 / 3.0) * here[gy][t]
                        + source_two[t][x, gy]
                        + (0.03125 * scale_two[t][x, gy]) * totals[gy][t]
                    )
                    write(x, gy, t, value)

        loop(8, T_TWO, body)

    def keep(x, gy, t, value):
        two[t][x, gy] = value

    def correct(pair, gy, t, value):
        for x in (2 * pair, 2 * pair + 1):
            level[t][x, gy] = level[t][x, gy] + value

    sweep_two(source_two, keep)
    sweep_two(two, correct)

    def last(x, _):
        here, totals = sides(level, x, 16, 2, only=1)
        gx, big = x >> 2, x & 3
        for gy in range(4):
            value = (1.0 / 3.0) * here[gy][0] + start_0[x, gy] + scale_0[x, gy] * totals[gy][0]
            out[gx * 4 + gy, pl.ds(pl.multiple_of(big * 8, 8), 8), :] = value

    loop(16, T_LAST, last)


def finish(second, got, out_hbm, out, sems):
    lane, row = lanes(), rows()
    even_lane, even_row = (lane & 1) == 0, (row & 1) == 0

    def group(g, _):
        for big in range(4):
            v = got[g, plane(big), :]
            pair = (
                jnp.where(even_lane, v, lroll(v, 1)),
                jnp.where(even_lane, lroll(v, 127), v),
            )
            for k in range(4):
                w = pair[k % 2]
                if k < 2:
                    w = jnp.where(even_row, w, sroll(w, 1))
                else:
                    w = jnp.where(even_row, sroll(w, 7), w)
                b = g * 4 + k
                for x in (2 * big, 2 * big + 1):
                    out[b, plane(x), :] = second[b, plane(x), :] + w
        return 0

    copies = []
    each = GROUPS // CHUNKS
    for i in range(CHUNKS):
        for g in range(i * each, (i + 1) * each):
            group(g, 0)
        part = pl.ds(i * (BANDS // CHUNKS), BANDS // CHUNKS)
        copies.append(pltpu.make_async_copy(out.at[part], out_hbm.at[part], sems.at[i]))
        copies[i].start()
    for copy in copies:
        copy.wait()


def swap(high, low, axis):
    size = lax.axis_size(axis)
    up = [(i, (i + 1) % size) for i in range(size)]
    return lax.ppermute(high, axis, up), lax.ppermute(low, axis, [(b, a) for a, b in up])


def in_hbm(array):
    return pltpu.with_memory_space_constraint(array, pltpu.HBM)


def local(orbitals, potential, centre, half_width):
    orb = orbitals.reshape(BANDS, 64, 128)
    pot = potential.reshape(64, 128)
    inverse = 1.0 / half_width
    face = shape(BANDS, 8, 128)
    thin, block = shape(9, 8, 128), shape(BANDS, 64, 128)

    xhi, xlo, pot = call(
        pack_x,
        [HBM] * 2,
        (face, face, shape(64, 128)),
        scratch=(pltpu.SemaphoreType.DMA((3,)),),
    )(in_hbm(orb), in_hbm(pot))
    yhi, ylo, zhi, zlo = call(pack_yz, [VMEM] * 2, (face, face, thin, thin))(orb, pot)
    zm, zp = swap(zhi, zlo, "gz")
    ym, yp = swap(yhi, ylo, "gy")
    xm, xp = swap(xhi, xlo, "gx")
    part, by_lane = call(
        first_inside, [SMEM] * 2 + [VMEM] * 2, (block, shape(2, 8, 128)), flops=BUSY
    )(centre, inverse, orb, pot)
    near = (pltpu.VMEM((64, 128), jnp.float32),)
    halos = (inverse, part, xm, xp, ym, yp, zm, zp)
    small = shape(GROUPS + 1, 8, 128)
    *faces, cxhi, cxlo, cyhi, cylo = call(
        first_faces, [SMEM] + [VMEM] * 7, (face,) * 4 + (small,) * 4, scratch=near
    )(*halos)
    cxm, cxp = swap(cxhi, cxlo, "gx")
    cym, cyp = swap(cyhi, cylo, "gy")
    (first,) = call(first_edges, [SMEM] + [VMEM] * 7, (block,), scratch=near, flops=BUSY)(*halos)
    buffer = (pltpu.VMEM((BANDS, 64, 128), jnp.float32), pltpu.SemaphoreType.DMA((CHUNKS,)))
    part, packed = call(
        second_inside,
        [SMEM] * 2 + [VMEM] * 3,
        (shape(4 * BANDS, 64, 128), shape(GROUPS, 40, 128)),
        out_specs=(HBM, VMEM),
        scratch=buffer,
        flops=BUSY,
        limit=48,
    )(centre, inverse, orb, pot, first)
    coarse, edge, xhi, xlo, yhi, ylo = call(
        coarse_edges,
        [SMEM] + [VMEM] * 15,
        (shape(GROUPS, 40, 128), shape(64, 128)) + (face,) * 4,
        out_specs=(HBM,) + (VMEM,) * 5,
        scratch=(pltpu.VMEM((GROUPS, 40, 128), jnp.float32), pltpu.SemaphoreType.DMA((2,))),
        aliases={12: 2, 13: 3, 14: 4, 15: 5},
    )(inverse, by_lane, pot, packed, cxm, cxp, cym, cyp, zm, zp, zhi, zlo, *faces)
    got = lax.all_to_all(coarse, ("gx", "gy"), 0, 0, tiled=True)
    xm, xp = swap(xhi, xlo, "gx")
    ym, yp = swap(yhi, ylo, "gy")
    (second,) = call(
        second_edges, [SMEM, HBM] + [VMEM] * 5, (block,), scratch=buffer, flops=BUSY, limit=48
    )(inverse, part, xm, xp, ym, yp, edge)
    ends = shape(10, 8, 128)
    mhi, mlo = call(pack_ends, [VMEM], (ends, ends))(got)
    left, right = swap(mhi, mlo, "gz")
    lines, half = (16, 4, 8, 128), (8, 4, 8, 128)
    terms = call(
        open_block, [VMEM], (shape(*lines),) * 4 + (shape(*half),), flops=BUSY
    )(got)
    lines, half = pltpu.VMEM(lines, jnp.float32), pltpu.VMEM(half, jnp.float32)
    (level,) = call(
        coarse_solve,
        [VMEM] * 8,
        (shape(GROUPS, 32, 128),),
        scratch=(lines,) * 4 + (half,) + (lines,) * 2 + (half,) * 4,
        limit=6,
    )(left, right, *terms, second)
    level = lax.all_to_all(level, ("gx", "gy"), 0, 0, tiled=True)
    (out,) = call(
        finish,
        [VMEM] * 2,
        (block,),
        out_specs=(HBM,),
        scratch=(pltpu.VMEM((BANDS, 64, 128), jnp.float32), pltpu.SemaphoreType.DMA((CHUNKS,))),
        limit=4,
    )(second, level)
    return out.reshape(BANDS, 8, 8, 128)


def solution(mesh):
    in_specs = (P(None, "gx", "gy", "gz"), P("gx", "gy", "gz"), P(), P())
    out_specs = P(None, "gx", "gy", "gz")
    return jax.shard_map(local, mesh=mesh, in_specs=in_specs, out_specs=out_specs, check_vma=False)
```

```python
import jax
import jax.numpy as jnp
from jax import lax
from jax.experimental import pallas as pl
from jax.experimental.pallas import tpu as pltpu
from jax.sharding import PartitionSpec as P

BANDS = 64
TILE = (8, 128)
GROUPS = 16
weight = 2.0 / 3.0

VMEM = pl.BlockSpec(memory_space=pltpu.VMEM)
SMEM = pl.BlockSpec(memory_space=pltpu.SMEM)
HBM = pl.BlockSpec(memory_space=pltpu.HBM)
CHUNKS = 4
BUSY = 400_000_000
T_REST_EDGE = 32
T_FIRST, T_INSIDE, T_EDGE, T_SECOND, T_PACK, T_SEND = 32, 16, 64, 16, 16, 8
T_OPEN, T_SWEEP, T_REST, T_TWO, T_LAST = 8, 16, 8, 8, 16


def shape(*dims):
    return jax.ShapeDtypeStruct(dims, jnp.float32)


def call(body, ins, outs, scratch=(), aliases=None, flops=4_000_000, limit=2, out_specs=None):
    return pl.pallas_call(
        body,
        out_shape=outs,
        in_specs=ins,
        out_specs=out_specs or tuple(VMEM for _ in outs),
        scratch_shapes=scratch,
        input_output_aliases=aliases or {},
        compiler_params=pltpu.CompilerParams(vmem_limit_bytes=limit * 1024 * 1024),
        cost_estimate=pl.CostEstimate(flops=flops, bytes_accessed=4_000_000, transcendentals=0),
    )


def lanes():
    return lax.broadcasted_iota(jnp.int32, TILE, 1)


def rows():
    return lax.broadcasted_iota(jnp.int32, TILE, 0)


def lroll(v, shift):
    return pltpu.roll(v, shift, 1)


def sroll(v, shift):
    return pltpu.roll(v, shift, 0)


def plane(x):
    return pl.ds(x * 8, 8)


def loop(count, step, body):
    def several(i, _):
        for k in range(step):
            body(i * step + k, 0)
        return 0

    lax.fori_loop(0, count // step, several, 0)


def nearest(lane, zp, zm, x):
    return jnp.where((lane & 1) == 0, zp[x], zm[x])


def pack_x(orb, pot_hbm, xhi, xlo, pot, sems):
    copies = (
        pltpu.make_async_copy(orb.at[:, plane(7), :], xhi, sems.at[0]),
        pltpu.make_async_copy(orb.at[:, plane(0), :], xlo, sems.at[1]),
        pltpu.make_async_copy(pot_hbm, pot, sems.at[2]),
    )
    for copy in copies:
        copy.start()
    for copy in copies:
        copy.wait()


def pack_yz(orb, pot, yhi, ylo, zhi, zlo):
    lane = lanes()

    def put(carry, v, slot):
        high, low = carry
        turned = lroll(v, (2 * slot + 2) & 127)
        high = jnp.where((lane >> 1) == slot, turned, high)
        low = jnp.where((lane >> 1) == ((slot + 1) & 63), turned, low)
        return high, low

    zero = jnp.zeros(TILE, jnp.float32)

    def body(i, carry):
        carry = list(carry)
        for k in range(T_FIRST):
            b = i * T_FIRST + k
            for x in range(8):
                carry[x] = put(carry[x], orb[b, plane(x), :], b)
            yhi[b] = orb[b, pl.ds(7, 8, stride=8), :]
            ylo[b] = orb[b, pl.ds(0, 8, stride=8), :]
        return tuple(carry)

    carry = lax.fori_loop(0, BANDS // T_FIRST, body, tuple((zero, zero) for _ in range(8)))
    for x in range(8):
        zhi[x] = carry[x][0]
        zlo[x] = lroll(carry[x][1], 126)
    edge = (zero, zero)
    for x in range(8):
        edge = put(edge, pot[plane(x), :], x)
    zhi[8] = edge[0]
    zlo[8] = lroll(edge[1], 126)


def inner_sum(get, x, lane, row):
    v = get(x)
    up = jnp.where(row == 7, 0.0, sroll(v, 7))
    down = jnp.where(row == 0, 0.0, sroll(v, 1))
    ahead = jnp.where(lane == 127, 0.0, lroll(v, 127))
    behind = jnp.where(lane == 0, 0.0, lroll(v, 1))
    total = (up + down) + (ahead + behind)
    if x > 0:
        total = total + get(x - 1)
    if x < 7:
        total = total + get(x + 1)
    return v, total


def outer_sum(x, b, xm, xp, ym, yp, halo, ends, row):
    total = jnp.where(ends, lroll(halo, 127 - 2 * b), 0.0)
    y = jnp.where(row == 0, ym[b, pl.ds(x, 1), :], yp[b, pl.ds(x, 1), :])
    total = total + jnp.where((row == 0) | (row == 7), y, 0.0)
    if x == 0:
        total = total + xm[b]
    if x == 7:
        total = total + xp[b]
    return total


def first_inside(middle, inverse, orb, pot, first, by_lane):
    lane, row = lanes(), rows()
    step = T_INSIDE

    def body(i, carry):
        lane_c, lane_r = carry
        for k in range(step):
            b = i * step + k
            c, r = middle[b], inverse[b]
            lane_c = jnp.where((lane >> 1) == b, c, lane_c)
            lane_r = jnp.where((lane >> 1) == b, r, lane_r)
            get = lambda x: orb[b, plane(x), :]
            for x in range(8):
                v, total = inner_sum(get, x, lane, row)
                first[b, plane(x), :] = (((3.0 - c) + pot[plane(x), :]) * v - 0.5 * total) * r
        return lane_c, lane_r

    zero = jnp.zeros(TILE, jnp.float32)
    by_lane[0], by_lane[1] = lax.fori_loop(0, BANDS // step, body, (zero, zero))


def pack_four(v, lane, row):
    even_lane, even_row = (lane & 1) == 0, (row & 1) == 0
    a = jnp.where(even_lane, v[0] + lroll(v[0], 127), v[1] + lroll(v[1], 1))
    b = jnp.where(even_lane, v[2] + lroll(v[2], 127), v[3] + lroll(v[3], 1))
    return jnp.where(even_row, a + sroll(a, 7), b + sroll(b, 1))


def first_faces(
    inverse, part, xm, xp, ym, yp, zm, zp, xhi, xlo, yhi, ylo, cxhi, cxlo, cyhi, cylo, near
):
    lane, row = lanes(), rows()
    ends = (lane == 0) | (lane == 127)
    for x in range(8):
        near[plane(x), :] = nearest(lane, zp, zm, x)

    def body(i, _):
        for k in range(T_EDGE):
            b = i * T_EDGE + k
            r = -0.5 * inverse[b]
            for x, out in ((0, xlo), (7, xhi)):
                total = outer_sum(x, b, xm, xp, ym, yp, near[plane(x), :], ends, row)
                out[b] = part[b, plane(x), :] + r * total
            for y, halo, out in ((0, ym, ylo), (7, yp, yhi)):
                cells = pl.ds(y, 8, stride=8)
                total = halo[b] + jnp.where(ends, lroll(near[cells, :], 127 - 2 * b), 0.0)
                side = jnp.where(row == 0, xm[b, pl.ds(y, 1), :], xp[b, pl.ds(y, 1), :])
                total = total + jnp.where((row == 0) | (row == 7), side, 0.0)
                out[b] = part[b, cells, :] + r * total
        return 0

    lax.fori_loop(0, BANDS // T_EDGE, body, 0)

    def coarsen(g, _):
        for face, out in ((xhi, cxhi), (xlo, cxlo), (yhi, cyhi), (ylo, cylo)):
            out[g] = pack_four([face[g * 4 + k] for k in range(4)], lane, row)

    loop(GROUPS, T_PACK, coarsen)
    cxhi[GROUPS] = near[plane(7), :]
    cxlo[GROUPS] = near[plane(0), :]
    cyhi[GROUPS] = near[pl.ds(7, 8, stride=8), :]
    cylo[GROUPS] = near[pl.ds(0, 8, stride=8), :]


def first_edges(inverse, part, xm, xp, ym, yp, zm, zp, first, near):
    lane, row = lanes(), rows()
    ends = (lane == 0) | (lane == 127)
    for x in range(8):
        near[plane(x), :] = nearest(lane, zp, zm, x)

    def body(i, _):
        for k in range(T_REST_EDGE):
            b = i * T_REST_EDGE + k
            r = -0.5 * inverse[b]
            for x in range(8):
                total = outer_sum(x, b, xm, xp, ym, yp, near[plane(x), :], ends, row)
                first[b, plane(x), :] = part[b, plane(x), :] + r * total
        return 0

    lax.fori_loop(0, BANDS // T_REST_EDGE, body, 0)


def chunk(i):
    return pl.ds(i * (BANDS // CHUNKS), BANDS // CHUNKS)


def second_inside(middle, inverse, orb, pot, first, second_hbm, packed, second, sems):
    lane, row = lanes(), rows()
    step = T_INSIDE

    def body(i, _):
        for k in range(step):
            b = i * step + k
            c, r = middle[b], 2.0 * inverse[b]
            get = lambda x: first[b, plane(x), :]
            for x in range(8):
                v, total = inner_sum(get, x, lane, row)
                value = (((3.0 - c) + pot[plane(x), :]) * v - 0.5 * total) * r
                second[b, plane(x), :] = value - orb[b, plane(x), :]
        return 0

    copies = []
    each = BANDS // CHUNKS // step
    for i in range(CHUNKS):
        lax.fori_loop(i * each, (i + 1) * each, body, 0)
        copies.append(pltpu.make_async_copy(second.at[chunk(i)], second_hbm.at[chunk(i)], sems.at[i]))
        copies[i].start()

    def coarsen(g, _):
        for big in range(4):
            low, high = plane(2 * big), plane(2 * big + 1)
            v = [second[g * 4 + k, low, :] + second[g * 4 + k, high, :] for k in range(4)]
            packed[g, plane(big), :] = 0.5 * pack_four(v, lane, row)

    loop(GROUPS, 8, coarsen)
    four = [pot[plane(2 * i), :] + pot[plane(2 * i + 1), :] for i in range(4)]
    pots = 0.125 * pack_four(four, lane, row)
    for g in range(GROUPS):
        packed[g, plane(4), :] = pots
    for copy in copies:
        copy.wait()


def coarse_edges(
    inverse, by_lane, pot, packed, ym, yp, xm, xp, zm, zp, zhi, zlo, face_0, face_1, face_2, face_3,
    coarse_hbm, edge, same_0, same_1, same_2, same_3, coarse, sems,
):
    lane, row = lanes(), rows()
    even_lane, even_row = (lane & 1) == 0, (row & 1) == 0

    cells = [nearest(lane, zp, zm, x) for x in range(8)]
    pots = nearest(lane, zp, zm, 8)
    values = []
    for x in range(8):
        v = cells[x]
        outer = jnp.where(even_lane, lroll(zp[x], 127), lroll(zm[x], 1))
        inner = jnp.where(even_lane, lroll(zhi[x], 127), lroll(zlo[x], 1))
        left = cells[x - 1] if x > 0 else xm[GROUPS]
        right = cells[x + 1] if x < 7 else xp[GROUPS]
        up = jnp.where(row == 7, yp[GROUPS, pl.ds(x, 1), :], sroll(v, 7))
        down = jnp.where(row == 0, ym[GROUPS, pl.ds(x, 1), :], sroll(v, 1))
        total = (left + right) + (up + down) + (outer + inner)
        here = jnp.where(even_lane, pots[:, 2 * x : 2 * x + 1], pots[:, 2 * x + 1 : 2 * x + 2])
        values.append(((3.0 - by_lane[0] + here) * v - 0.5 * total) * by_lane[1])
        edge[plane(x), :] = values[x]

    ends = []
    for big in range(4):
        v = values[2 * big] + values[2 * big + 1]
        v = v + jnp.where(even_row, sroll(v, 7), sroll(v, 1))
        place = lane & 3
        ends.append(jnp.where(place == 1, lroll(v, 127), jnp.where(place == 2, lroll(v, 1), v)))
    outside = (lane < 2) | (lane >= 126)

    def group(g, _):
        r = [inverse[g * 4 + k] for k in range(4)]
        half = -0.5 * jnp.where(
            even_row, jnp.where(even_lane, r[0], r[1]), jnp.where(even_lane, r[2], r[3])
        )
        for big in range(4):
            z = jnp.where(
                even_row,
                lroll(ends[big], (254 - 8 * g) & 127),
                lroll(ends[big], (250 - 8 * g) & 127),
            )
            y = jnp.where(row < 2, sroll(ym[g], (8 - 2 * big) % 8), sroll(yp[g], 6 - 2 * big))
            total = jnp.where(outside, z, 0.0) + jnp.where((row < 2) | (row >= 6), y, 0.0)
            if big == 0:
                total = total + xm[g]
            if big == 3:
                total = total + xp[g]
            coarse[g, plane(big), :] = packed[g, plane(big), :] + half * total
        coarse[g, plane(4), :] = packed[g, plane(4), :]

    copies = []
    for i in range(2):
        for g in range(8 * i, 8 * i + 8):
            group(g, 0)
        half = pl.ds(8 * i, 8)
        copies.append(pltpu.make_async_copy(coarse.at[half], coarse_hbm.at[half], sems.at[i]))
        copies[i].start()
    for copy in copies:
        copy.wait()


def second_edges(inverse, part_hbm, xm, xp, ym, yp, edge, after, second, part, sems):
    lane, row = lanes(), rows()
    ends = (lane == 0) | (lane == 127)
    copies = []
    for i in range(CHUNKS):
        copies.append(pltpu.make_async_copy(part_hbm.at[chunk(i)], part.at[chunk(i)], sems.at[i]))
        copies[i].start()

    def body(i, _):
        for k in range(T_SECOND):
            b = i * T_SECOND + k
            r = inverse[b]
            for x in range(8):
                total = outer_sum(x, b, xm, xp, ym, yp, edge[plane(x), :], ends, row)
                second[b, plane(x), :] = part[b, plane(x), :] - r * total
        return 0

    each = BANDS // CHUNKS // T_SECOND
    for i in range(CHUNKS):
        copies[i].wait()
        lax.fori_loop(i * each, (i + 1) * each, body, 0)


def pack_ends(got, mhi, mlo):
    lane = lanes()
    zero = jnp.zeros(TILE, jnp.float32)

    def send(half, _):
        high = low = zero
        for odd in range(2):
            for big in range(4):
                v = got[2 * half + odd, plane(big), :]
                mine = (lane >> 4) == 2 * big + odd
                at = 32 * big + 16 * odd
                high = jnp.where(mine, lroll(v, (at + 16) & 127), high)
                low = jnp.where(mine, lroll(v, at), low)
        mhi[half] = high
        mlo[half] = low

    loop(GROUPS // 2, T_SEND, send)
    for half in range(2):
        high = low = zero
        for i in range(8):
            v = got[8 * half + i, plane(4), :]
            high = jnp.where((lane >> 4) == i, lroll(v, (16 * i + 16) & 127), high)
            low = jnp.where((lane >> 4) == i, lroll(v, 16 * i), low)
        mhi[8 + half] = high
        mlo[8 + half] = low


def coarse_terms(blocks, pots, gx, gy, source, diagonal, scale, start, scale_two):
    lane, row = lanes(), rows()
    even_lane, even_row = (lane & 1) == 0, (row & 1) == 0
    a = jnp.where(even_lane, pots, lroll(pots, 1))
    b = jnp.where(even_lane, lroll(pots, 127), pots)
    each = []
    for up in (False, True):
        for w in (a, b):
            each.append(jnp.where(even_row, sroll(w, 7), w) if up else jnp.where(even_row, w, sroll(w, 1)))
    for big in range(4):
        at = (gx * 4 + big, gy)
        d = each[big] + 0.8
        w = weight / d
        source[at] = blocks[big]
        diagonal[at] = d
        scale[at] = 0.125 * w
        start[at] = w * blocks[big]
    for k in range(2):
        p = 0.125 * pair_sum(each[2 * k] + each[2 * k + 1], lane, row)
        scale_two[gx * 2 + k, gy] = weight / (p + 0.2375)


def pair_sum(v, lane, row):
    v = v + jnp.where((row & 2) == 0, sroll(v, 6), sroll(v, 2))
    return v + jnp.where((lane & 2) == 0, lroll(v, 126), lroll(v, 2))


def open_block(got, source, diagonal, scale, start, scale_two):
    def unpack(src, _):
        blocks = [got[src, plane(big), :] for big in range(4)]
        pots = got[src, plane(4), :]
        coarse_terms(blocks, pots, src >> 2, src & 3, source, diagonal, scale, start, scale_two)

    loop(GROUPS, T_OPEN, unpack)


def coarse_solve(
    left, right, source_0, diagonal_0, scale_0, start_0, scale_two_0, second, out,
    source_1, diagonal_1, scale_1, start_1, scale_two_1,
    level_0, level_1, source_two_0, source_two_1, two_0, two_1,
):
    lane, row = lanes(), rows()
    source, diagonal = (source_0, source_1), (diagonal_0, diagonal_1)
    scale, start = (scale_0, scale_1), (start_0, start_1)
    scale_two, level = (scale_two_0, scale_two_1), (level_0, level_1)
    source_two, two = (source_two_0, source_two_1), (two_0, two_1)

    def unpack(group, _):
        for i in range(8):
            src = 8 * group + i
            a, b = left[4 * group + i // 2], right[4 * group + i // 2]
            if i % 2 == 0:
                b = lroll(b, 16)
            else:
                a = lroll(a, 112)
            halo = jnp.where(((lane >> 4) & 1) == 0, a, b)
            blocks = [lroll(halo, 112 - 32 * big) for big in range(4)]
            near, far = right[8 + group], left[8 + group]
            pots = jnp.where(lane < 64, lroll(near, (128 - 16 * i) & 127), lroll(far, 112 - 16 * i))
            coarse_terms(
                blocks, pots, 2 * group + i // 4, i % 4,
                source_1, diagonal_1, scale_1, start_1, scale_two_1,
            )

    loop(2, 1, unpack)

    def load(ref, x):
        return [[ref[t][x, gy] for t in range(2)] for gy in range(4)]

    def sides(ref, x, count, step, only=2):
        here = load(ref, x)
        before = lax.rem(x + (count - 1), count)
        after = lax.rem(x + 1, count)
        down = [[sroll(here[gy][t], step) for t in range(2)] for gy in range(4)]
        up = [[sroll(here[gy][t], 8 - step) for t in range(2)] for gy in range(4)] if step != 4 else down
        behind = [[lroll(here[gy][t], step) for t in range(2)] for gy in range(4)]
        ahead = [[lroll(here[gy][t], 128 - step) for t in range(2)] for gy in range(4)]
        totals = []
        for gy in range(4):
            line = []
            for t in range(only):
                total = ref[t][before, gy] + ref[t][after, gy]
                y = jnp.where(row < step, down[(gy + 3) % 4][t], down[gy][t])
                y = y + jnp.where(row >= 8 - step, up[(gy + 1) % 4][t], up[gy][t])
                z = jnp.where(lane < step, behind[gy][1 - t], behind[gy][t])
                z = z + jnp.where(lane >= 128 - step, ahead[gy][1 - t], ahead[gy][t])
                line.append(total + y + z)
            totals.append(line)
        return here, totals

    def sweep_one(x, _):
        here, totals = sides(start, x, 16, 2)
        for gy in range(4):
            for t in range(2):
                value = (4.0 / 3.0) * here[gy][t] + scale[t][x, gy] * totals[gy][t]
                level[t][x, gy] = value

    loop(16, T_SWEEP, sweep_one)

    def residue(pair, _):
        sums = [[None, None] for _ in range(4)]
        for k in range(2):
            x = 2 * pair + k
            here, totals = sides(level, x, 16, 2)
            for gy in range(4):
                for t in range(2):
                    r = source[t][x, gy] - (
                        diagonal[t][x, gy] * here[gy][t] - 0.125 * totals[gy][t]
                    )
                    sums[gy][t] = r if k == 0 else sums[gy][t] + r
        for gy in range(4):
            for t in range(2):
                r = 0.5 * pair_sum(sums[gy][t], lane, row)
                source_two[t][pair, gy] = scale_two[t][pair, gy] * r

    loop(8, T_REST, residue)

    def sweep_two(old, write):
        def body(x, _):
            here, totals = sides(old, x, 8, 4)
            for gy in range(4):
                for t in range(2):
                    value = (
                        (1.0 / 3.0) * here[gy][t]
                        + source_two[t][x, gy]
                        + (0.03125 * scale_two[t][x, gy]) * totals[gy][t]
                    )
                    write(x, gy, t, value)

        loop(8, T_TWO, body)

    def keep(x, gy, t, value):
        two[t][x, gy] = value

    def correct(pair, gy, t, value):
        for x in (2 * pair, 2 * pair + 1):
            level[t][x, gy] = level[t][x, gy] + value

    sweep_two(source_two, keep)
    sweep_two(two, correct)

    def last(x, _):
        here, totals = sides(level, x, 16, 2, only=1)
        gx, big = x >> 2, x & 3
        for gy in range(4):
            value = (1.0 / 3.0) * here[gy][0] + start_0[x, gy] + scale_0[x, gy] * totals[gy][0]
            out[gx * 4 + gy, pl.ds(pl.multiple_of(big * 8, 8), 8), :] = value

    loop(16, T_LAST, last)


def finish(second, got, out_hbm, out, sems):
    lane, row = lanes(), rows()
    even_lane, even_row = (lane & 1) == 0, (row & 1) == 0

    def group(g, _):
        for big in range(4):
            v = got[g, plane(big), :]
            pair = (
                jnp.where(even_lane, v, lroll(v, 1)),
                jnp.where(even_lane, lroll(v, 127), v),
            )
            for k in range(4):
                w = pair[k % 2]
                if k < 2:
                    w = jnp.where(even_row, w, sroll(w, 1))
                else:
                    w = jnp.where(even_row, sroll(w, 7), w)
                b = g * 4 + k
                for x in (2 * big, 2 * big + 1):
                    out[b, plane(x), :] = second[b, plane(x), :] + w
        return 0

    copies = []
    each = GROUPS // CHUNKS
    for i in range(CHUNKS):
        for g in range(i * each, (i + 1) * each):
            group(g, 0)
        part = pl.ds(i * (BANDS // CHUNKS), BANDS // CHUNKS)
        copies.append(pltpu.make_async_copy(out.at[part], out_hbm.at[part], sems.at[i]))
        copies[i].start()
    for copy in copies:
        copy.wait()


def swap(high, low, axis):
    size = lax.axis_size(axis)
    up = [(i, (i + 1) % size) for i in range(size)]
    return lax.ppermute(high, axis, up), lax.ppermute(low, axis, [(b, a) for a, b in up])


def in_hbm(array):
    return pltpu.with_memory_space_constraint(array, pltpu.HBM)


def local(orbitals, potential, centre, half_width):
    orb = orbitals.reshape(BANDS, 64, 128)
    pot = potential.reshape(64, 128)
    inverse = 1.0 / half_width
    face = shape(BANDS, 8, 128)
    thin, block = shape(9, 8, 128), shape(BANDS, 64, 128)

    xhi, xlo, pot = call(
        pack_x,
        [HBM] * 2,
        (face, face, shape(64, 128)),
        scratch=(pltpu.SemaphoreType.DMA((3,)),),
    )(in_hbm(orb), in_hbm(pot))
    yhi, ylo, zhi, zlo = call(pack_yz, [VMEM] * 2, (face, face, thin, thin))(orb, pot)
    zm, zp = swap(zhi, zlo, "gz")
    ym, yp = swap(yhi, ylo, "gy")
    xm, xp = swap(xhi, xlo, "gx")
    part, by_lane = call(
        first_inside, [SMEM] * 2 + [VMEM] * 2, (block, shape(2, 8, 128)), flops=BUSY
    )(centre, inverse, orb, pot)
    near = (pltpu.VMEM((64, 128), jnp.float32),)
    halos = (inverse, part, xm, xp, ym, yp, zm, zp)
    small = shape(GROUPS + 1, 8, 128)
    *faces, cxhi, cxlo, cyhi, cylo = call(
        first_faces, [SMEM] + [VMEM] * 7, (face,) * 4 + (small,) * 4, scratch=near
    )(*halos)
    cxm, cxp = swap(cxhi, cxlo, "gx")
    cym, cyp = swap(cyhi, cylo, "gy")
    (first,) = call(first_edges, [SMEM] + [VMEM] * 7, (block,), scratch=near, flops=BUSY)(*halos)
    buffer = (pltpu.VMEM((BANDS, 64, 128), jnp.float32), pltpu.SemaphoreType.DMA((CHUNKS,)))
    part, packed = call(
        second_inside,
        [SMEM] * 2 + [VMEM] * 3,
        (shape(4 * BANDS, 64, 128), shape(GROUPS, 40, 128)),
        out_specs=(HBM, VMEM),
        scratch=buffer,
        flops=BUSY,
        limit=48,
    )(centre, inverse, orb, pot, first)
    coarse, edge, xhi, xlo, yhi, ylo = call(
        coarse_edges,
        [SMEM] + [VMEM] * 15,
        (shape(GROUPS, 40, 128), shape(64, 128)) + (face,) * 4,
        out_specs=(HBM,) + (VMEM,) * 5,
        scratch=(pltpu.VMEM((GROUPS, 40, 128), jnp.float32), pltpu.SemaphoreType.DMA((2,))),
        aliases={12: 2, 13: 3, 14: 4, 15: 5},
    )(inverse, by_lane, pot, packed, cym, cyp, cxm, cxp, zm, zp, zhi, zlo, *faces)
    got = lax.all_to_all(coarse, ("gx", "gy"), 0, 0, tiled=True)
    xm, xp = swap(xhi, xlo, "gx")
    ym, yp = swap(yhi, ylo, "gy")
    ends = shape(10, 8, 128)
    mhi, mlo = call(pack_ends, [VMEM], (ends, ends))(got)
    left, right = swap(mhi, mlo, "gz")
    lines, half = (16, 4, 8, 128), (8, 4, 8, 128)
    terms = call(
        open_block, [VMEM], (shape(*lines),) * 4 + (shape(*half),), flops=BUSY
    )(got)
    (second,) = call(
        second_edges, [SMEM, HBM] + [VMEM] * 6, (block,), scratch=buffer, flops=BUSY, limit=48
    )(inverse, part, xm, xp, ym, yp, edge, terms[4])
    lines, half = pltpu.VMEM(lines, jnp.float32), pltpu.VMEM(half, jnp.float32)
    (level,) = call(
        coarse_solve,
        [VMEM] * 8,
        (shape(GROUPS, 32, 128),),
        scratch=(lines,) * 4 + (half,) + (lines,) * 2 + (half,) * 4,
        limit=6,
    )(left, right, *terms, second)
    level = lax.all_to_all(level, ("gx", "gy"), 0, 0, tiled=True)
    (out,) = call(
        finish,
        [VMEM] * 2,
        (block,),
        out_specs=(HBM,),
        scratch=(pltpu.VMEM((BANDS, 64, 128), jnp.float32), pltpu.SemaphoreType.DMA((CHUNKS,))),
        limit=4,
    )(second, level)
    return out.reshape(BANDS, 8, 8, 128)


def solution(mesh):
    in_specs = (P(None, "gx", "gy", "gz"), P("gx", "gy", "gz"), P(), P())
    out_specs = P(None, "gx", "gy", "gz")
    return jax.shard_map(local, mesh=mesh, in_specs=in_specs, out_specs=out_specs, check_vma=False)
```

```python
import jax
import jax.numpy as jnp
from jax import lax
from jax.experimental import pallas as pl
from jax.experimental.pallas import tpu as pltpu
from jax.sharding import PartitionSpec as P

BANDS = 64
TILE = (8, 128)
GROUPS = 16
weight = 2.0 / 3.0

VMEM = pl.BlockSpec(memory_space=pltpu.VMEM)
SMEM = pl.BlockSpec(memory_space=pltpu.SMEM)
HBM = pl.BlockSpec(memory_space=pltpu.HBM)
ANY = pl.BlockSpec(memory_space=pl.ANY)
CHUNKS = 4
BUSY = 400_000_000
T_REST_EDGE = 32
T_FIRST, T_INSIDE, T_EDGE, T_SECOND, T_PACK, T_SEND = 32, 16, 64, 16, 16, 8
T_OPEN, T_SWEEP, T_REST, T_TWO, T_LAST = 8, 16, 8, 8, 16


def shape(*dims):
    return jax.ShapeDtypeStruct(dims, jnp.float32)


def call(body, ins, outs, scratch=(), aliases=None, flops=4_000_000, limit=2, out_specs=None):
    return pl.pallas_call(
        body,
        out_shape=outs,
        in_specs=ins,
        out_specs=out_specs or tuple(VMEM for _ in outs),
        scratch_shapes=scratch,
        input_output_aliases=aliases or {},
        compiler_params=pltpu.CompilerParams(vmem_limit_bytes=limit * 1024 * 1024),
        cost_estimate=pl.CostEstimate(flops=flops, bytes_accessed=4_000_000, transcendentals=0),
    )


def lanes():
    return lax.broadcasted_iota(jnp.int32, TILE, 1)


def rows():
    return lax.broadcasted_iota(jnp.int32, TILE, 0)


def lroll(v, shift):
    return pltpu.roll(v, shift, 1)


def sroll(v, shift):
    return pltpu.roll(v, shift, 0)


def plane(x):
    return pl.ds(x * 8, 8)


def loop(count, step, body):
    def several(i, _):
        for k in range(step):
            body(i * step + k, 0)
        return 0

    lax.fori_loop(0, count // step, several, 0)


def nearest(lane, zp, zm, x):
    return jnp.where((lane & 1) == 0, zp[x], zm[x])


def pack_x(orb, pot_hbm, xhi, xlo, pot, sems):
    copies = (
        pltpu.make_async_copy(orb.at[:, plane(7), :], xhi, sems.at[0]),
        pltpu.make_async_copy(orb.at[:, plane(0), :], xlo, sems.at[1]),
        pltpu.make_async_copy(pot_hbm, pot, sems.at[2]),
    )
    for copy in copies:
        copy.start()
    for copy in copies:
        copy.wait()


def pack_yz(orb, pot, yhi, ylo, zhi, zlo):
    lane = lanes()

    def put(carry, v, slot):
        high, low = carry
        turned = lroll(v, (2 * slot + 2) & 127)
        high = jnp.where((lane >> 1) == slot, turned, high)
        low = jnp.where((lane >> 1) == ((slot + 1) & 63), turned, low)
        return high, low

    zero = jnp.zeros(TILE, jnp.float32)

    def body(i, carry):
        carry = list(carry)
        for k in range(T_FIRST):
            b = i * T_FIRST + k
            for x in range(8):
                carry[x] = put(carry[x], orb[b, plane(x), :], b)
            yhi[b] = orb[b, pl.ds(7, 8, stride=8), :]
            ylo[b] = orb[b, pl.ds(0, 8, stride=8), :]
        return tuple(carry)

    carry = lax.fori_loop(0, BANDS // T_FIRST, body, tuple((zero, zero) for _ in range(8)))
    for x in range(8):
        zhi[x] = carry[x][0]
        zlo[x] = lroll(carry[x][1], 126)
    edge = (zero, zero)
    for x in range(8):
        edge = put(edge, pot[plane(x), :], x)
    zhi[8] = edge[0]
    zlo[8] = lroll(edge[1], 126)


def inner_sum(get, x, lane, row):
    v = get(x)
    up = jnp.where(row == 7, 0.0, sroll(v, 7))
    down = jnp.where(row == 0, 0.0, sroll(v, 1))
    ahead = jnp.where(lane == 127, 0.0, lroll(v, 127))
    behind = jnp.where(lane == 0, 0.0, lroll(v, 1))
    total = (up + down) + (ahead + behind)
    if x > 0:
        total = total + get(x - 1)
    if x < 7:
        total = total + get(x + 1)
    return v, total


def outer_sum(x, b, xm, xp, ym, yp, halo, ends, row):
    total = jnp.where(ends, lroll(halo, 127 - 2 * b), 0.0)
    y = jnp.where(row == 0, ym[b, pl.ds(x, 1), :], yp[b, pl.ds(x, 1), :])
    total = total + jnp.where((row == 0) | (row == 7), y, 0.0)
    if x == 0:
        total = total + xm[b]
    if x == 7:
        total = total + xp[b]
    return total


def first_inside(middle, inverse, orb, pot, first, by_lane):
    lane, row = lanes(), rows()
    step = T_INSIDE

    def body(i, carry):
        lane_c, lane_r = carry
        for k in range(step):
            b = i * step + k
            c, r = middle[b], inverse[b]
            lane_c = jnp.where((lane >> 1) == b, c, lane_c)
            lane_r = jnp.where((lane >> 1) == b, r, lane_r)
            get = lambda x: orb[b, plane(x), :]
            for x in range(8):
                v, total = inner_sum(get, x, lane, row)
                first[b, plane(x), :] = (((3.0 - c) + pot[plane(x), :]) * v - 0.5 * total) * r
        return lane_c, lane_r

    zero = jnp.zeros(TILE, jnp.float32)
    by_lane[0], by_lane[1] = lax.fori_loop(0, BANDS // step, body, (zero, zero))


def pack_four(v, lane, row):
    even_lane, even_row = (lane & 1) == 0, (row & 1) == 0
    a = jnp.where(even_lane, v[0] + lroll(v[0], 127), v[1] + lroll(v[1], 1))
    b = jnp.where(even_lane, v[2] + lroll(v[2], 127), v[3] + lroll(v[3], 1))
    return jnp.where(even_row, a + sroll(a, 7), b + sroll(b, 1))


def first_faces(
    inverse, part, xm, xp, ym, yp, zm, zp, xhi, xlo, yhi, ylo, cxhi, cxlo, cyhi, cylo, near
):
    lane, row = lanes(), rows()
    ends = (lane == 0) | (lane == 127)
    for x in range(8):
        near[plane(x), :] = nearest(lane, zp, zm, x)

    def body(i, _):
        for k in range(T_EDGE):
            b = i * T_EDGE + k
            r = -0.5 * inverse[b]
            for x, out in ((0, xlo), (7, xhi)):
                total = outer_sum(x, b, xm, xp, ym, yp, near[plane(x), :], ends, row)
                out[b] = part[b, plane(x), :] + r * total
            for y, halo, out in ((0, ym, ylo), (7, yp, yhi)):
                cells = pl.ds(y, 8, stride=8)
                total = halo[b] + jnp.where(ends, lroll(near[cells, :], 127 - 2 * b), 0.0)
                side = jnp.where(row == 0, xm[b, pl.ds(y, 1), :], xp[b, pl.ds(y, 1), :])
                total = total + jnp.where((row == 0) | (row == 7), side, 0.0)
                out[b] = part[b, cells, :] + r * total
        return 0

    lax.fori_loop(0, BANDS // T_EDGE, body, 0)

    def coarsen(g, _):
        for face, out in ((xhi, cxhi), (xlo, cxlo), (yhi, cyhi), (ylo, cylo)):
            out[g] = pack_four([face[g * 4 + k] for k in range(4)], lane, row)

    loop(GROUPS, T_PACK, coarsen)
    cxhi[GROUPS] = near[plane(7), :]
    cxlo[GROUPS] = near[plane(0), :]
    cyhi[GROUPS] = near[pl.ds(7, 8, stride=8), :]
    cylo[GROUPS] = near[pl.ds(0, 8, stride=8), :]


def first_edges(inverse, part, xm, xp, ym, yp, zm, zp, first, near):
    lane, row = lanes(), rows()
    ends = (lane == 0) | (lane == 127)
    for x in range(8):
        near[plane(x), :] = nearest(lane, zp, zm, x)

    def body(i, _):
        for k in range(T_REST_EDGE):
            b = i * T_REST_EDGE + k
            r = -0.5 * inverse[b]
            for x in range(8):
                total = outer_sum(x, b, xm, xp, ym, yp, near[plane(x), :], ends, row)
                first[b, plane(x), :] = part[b, plane(x), :] + r * total
        return 0

    lax.fori_loop(0, BANDS // T_REST_EDGE, body, 0)


def chunk(i):
    return pl.ds(i * (BANDS // CHUNKS), BANDS // CHUNKS)


def second_inside(middle, inverse, orb, pot, first, second_hbm, packed, second, sems):
    lane, row = lanes(), rows()
    step = T_INSIDE

    def body(i, _):
        for k in range(step):
            b = i * step + k
            c, r = middle[b], 2.0 * inverse[b]
            get = lambda x: first[b, plane(x), :]
            for x in range(8):
                v, total = inner_sum(get, x, lane, row)
                value = (((3.0 - c) + pot[plane(x), :]) * v - 0.5 * total) * r
                second[b, plane(x), :] = value - orb[b, plane(x), :]
        return 0

    copies = []
    each = BANDS // CHUNKS // step
    for i in range(CHUNKS):
        lax.fori_loop(i * each, (i + 1) * each, body, 0)
        copies.append(pltpu.make_async_copy(second.at[chunk(i)], second_hbm.at[chunk(i)], sems.at[i]))
        copies[i].start()

    def coarsen(g, _):
        for big in range(4):
            low, high = plane(2 * big), plane(2 * big + 1)
            v = [second[g * 4 + k, low, :] + second[g * 4 + k, high, :] for k in range(4)]
            packed[g, plane(big), :] = 0.5 * pack_four(v, lane, row)

    loop(GROUPS, 8, coarsen)
    four = [pot[plane(2 * i), :] + pot[plane(2 * i + 1), :] for i in range(4)]
    pots = 0.125 * pack_four(four, lane, row)
    for g in range(GROUPS):
        packed[g, plane(4), :] = pots
    for copy in copies:
        copy.wait()


def coarse_edges(
    inverse, by_lane, pot, packed, xm, xp, ym, yp, zm, zp, zhi, zlo, face_0, face_1, face_2, face_3,
    coarse_hbm, edge, same_0, same_1, same_2, same_3, coarse, sems,
):
    lane, row = lanes(), rows()
    even_lane, even_row = (lane & 1) == 0, (row & 1) == 0

    cells = [nearest(lane, zp, zm, x) for x in range(8)]
    pots = nearest(lane, zp, zm, 8)
    values = []
    for x in range(8):
        v = cells[x]
        outer = jnp.where(even_lane, lroll(zp[x], 127), lroll(zm[x], 1))
        inner = jnp.where(even_lane, lroll(zhi[x], 127), lroll(zlo[x], 1))
        left = cells[x - 1] if x > 0 else xm[GROUPS]
        right = cells[x + 1] if x < 7 else xp[GROUPS]
        up = jnp.where(row == 7, yp[GROUPS, pl.ds(x, 1), :], sroll(v, 7))
        down = jnp.where(row == 0, ym[GROUPS, pl.ds(x, 1), :], sroll(v, 1))
        total = (left + right) + (up + down) + (outer + inner)
        here = jnp.where(even_lane, pots[:, 2 * x : 2 * x + 1], pots[:, 2 * x + 1 : 2 * x + 2])
        values.append(((3.0 - by_lane[0] + here) * v - 0.5 * total) * by_lane[1])
        edge[plane(x), :] = values[x]

    ends = []
    for big in range(4):
        v = values[2 * big] + values[2 * big + 1]
        v = v + jnp.where(even_row, sroll(v, 7), sroll(v, 1))
        place = lane & 3
        ends.append(jnp.where(place == 1, lroll(v, 127), jnp.where(place == 2, lroll(v, 1), v)))
    outside = (lane < 2) | (lane >= 126)

    def group(g, _):
        r = [inverse[g * 4 + k] for k in range(4)]
        half = -0.5 * jnp.where(
            even_row, jnp.where(even_lane, r[0], r[1]), jnp.where(even_lane, r[2], r[3])
        )
        for big in range(4):
            z = jnp.where(
                even_row,
                lroll(ends[big], (254 - 8 * g) & 127),
                lroll(ends[big], (250 - 8 * g) & 127),
            )
            y = jnp.where(row < 2, sroll(ym[g], (8 - 2 * big) % 8), sroll(yp[g], 6 - 2 * big))
            total = jnp.where(outside, z, 0.0) + jnp.where((row < 2) | (row >= 6), y, 0.0)
            if big == 0:
                total = total + xm[g]
            if big == 3:
                total = total + xp[g]
            coarse[g, plane(big), :] = packed[g, plane(big), :] + half * total
        coarse[g, plane(4), :] = packed[g, plane(4), :]

    copies = []
    for i in range(2):
        for g in range(8 * i, 8 * i + 8):
            group(g, 0)
        half = pl.ds(8 * i, 8)
        copies.append(pltpu.make_async_copy(coarse.at[half], coarse_hbm.at[half], sems.at[i]))
        copies[i].start()
    for copy in copies:
        copy.wait()


def second_edges(inverse, part_hbm, xm, xp, ym, yp, edge, second, part, sems):
    lane, row = lanes(), rows()
    ends = (lane == 0) | (lane == 127)
    copies = []
    for i in range(CHUNKS):
        copies.append(pltpu.make_async_copy(part_hbm.at[chunk(i)], part.at[chunk(i)], sems.at[i]))
        copies[i].start()

    def body(i, _):
        for k in range(T_SECOND):
            b = i * T_SECOND + k
            r = inverse[b]
            for x in range(8):
                total = outer_sum(x, b, xm, xp, ym, yp, edge[plane(x), :], ends, row)
                second[b, plane(x), :] = part[b, plane(x), :] - r * total
        return 0

    each = BANDS // CHUNKS // T_SECOND
    for i in range(CHUNKS):
        copies[i].wait()
        lax.fori_loop(i * each, (i + 1) * each, body, 0)


def pack_ends(got, mhi, mlo):
    lane = lanes()
    zero = jnp.zeros(TILE, jnp.float32)

    def send(half, _):
        high = low = zero
        for odd in range(2):
            for big in range(4):
                v = got[2 * half + odd, plane(big), :]
                mine = (lane >> 4) == 2 * big + odd
                at = 32 * big + 16 * odd
                high = jnp.where(mine, lroll(v, (at + 16) & 127), high)
                low = jnp.where(mine, lroll(v, at), low)
        mhi[half] = high
        mlo[half] = low

    loop(GROUPS // 2, T_SEND, send)
    for half in range(2):
        high = low = zero
        for i in range(8):
            v = got[8 * half + i, plane(4), :]
            high = jnp.where((lane >> 4) == i, lroll(v, (16 * i + 16) & 127), high)
            low = jnp.where((lane >> 4) == i, lroll(v, 16 * i), low)
        mhi[8 + half] = high
        mlo[8 + half] = low


def coarse_terms(blocks, pots, gx, gy, source, diagonal, scale, start, scale_two):
    lane, row = lanes(), rows()
    even_lane, even_row = (lane & 1) == 0, (row & 1) == 0
    a = jnp.where(even_lane, pots, lroll(pots, 1))
    b = jnp.where(even_lane, lroll(pots, 127), pots)
    each = []
    for up in (False, True):
        for w in (a, b):
            each.append(jnp.where(even_row, sroll(w, 7), w) if up else jnp.where(even_row, w, sroll(w, 1)))
    for big in range(4):
        at = (gx * 4 + big, gy)
        d = each[big] + 0.8
        w = weight / d
        source[at] = blocks[big]
        diagonal[at] = d
        scale[at] = 0.125 * w
        start[at] = w * blocks[big]
    for k in range(2):
        p = 0.125 * pair_sum(each[2 * k] + each[2 * k + 1], lane, row)
        scale_two[gx * 2 + k, gy] = weight / (p + 0.2375)


def pair_sum(v, lane, row):
    v = v + jnp.where((row & 2) == 0, sroll(v, 6), sroll(v, 2))
    return v + jnp.where((lane & 2) == 0, lroll(v, 126), lroll(v, 2))


def open_block(got, source, diagonal, scale, start, scale_two):
    def unpack(src, _):
        blocks = [got[src, plane(big), :] for big in range(4)]
        pots = got[src, plane(4), :]
        coarse_terms(blocks, pots, src >> 2, src & 3, source, diagonal, scale, start, scale_two)

    loop(GROUPS, T_OPEN, unpack)


def coarse_solve(
    left, right, source_0, diagonal_0, scale_0, start_0, scale_two_0, second, out,
    source_1, diagonal_1, scale_1, start_1, scale_two_1,
    level_0, level_1, source_two_0, source_two_1, two_0, two_1,
):
    lane, row = lanes(), rows()
    source, diagonal = (source_0, source_1), (diagonal_0, diagonal_1)
    scale, start = (scale_0, scale_1), (start_0, start_1)
    scale_two, level = (scale_two_0, scale_two_1), (level_0, level_1)
    source_two, two = (source_two_0, source_two_1), (two_0, two_1)

    def unpack(group, _):
        for i in range(8):
            src = 8 * group + i
            a, b = left[4 * group + i // 2], right[4 * group + i // 2]
            if i % 2 == 0:
                b = lroll(b, 16)
            else:
                a = lroll(a, 112)
            halo = jnp.where(((lane >> 4) & 1) == 0, a, b)
            blocks = [lroll(halo, 112 - 32 * big) for big in range(4)]
            near, far = right[8 + group], left[8 + group]
            pots = jnp.where(lane < 64, lroll(near, (128 - 16 * i) & 127), lroll(far, 112 - 16 * i))
            coarse_terms(
                blocks, pots, 2 * group + i // 4, i % 4,
                source_1, diagonal_1, scale_1, start_1, scale_two_1,
            )

    loop(2, 1, unpack)

    def load(ref, x):
        return [[ref[t][x, gy] for t in range(2)] for gy in range(4)]

    def sides(ref, x, count, step, only=2):
        here = load(ref, x)
        before = lax.rem(x + (count - 1), count)
        after = lax.rem(x + 1, count)
        down = [[sroll(here[gy][t], step) for t in range(2)] for gy in range(4)]
        up = [[sroll(here[gy][t], 8 - step) for t in range(2)] for gy in range(4)] if step != 4 else down
        behind = [[lroll(here[gy][t], step) for t in range(2)] for gy in range(4)]
        ahead = [[lroll(here[gy][t], 128 - step) for t in range(2)] for gy in range(4)]
        totals = []
        for gy in range(4):
            line = []
            for t in range(only):
                total = ref[t][before, gy] + ref[t][after, gy]
                y = jnp.where(row < step, down[(gy + 3) % 4][t], down[gy][t])
                y = y + jnp.where(row >= 8 - step, up[(gy + 1) % 4][t], up[gy][t])
                z = jnp.where(lane < step, behind[gy][1 - t], behind[gy][t])
                z = z + jnp.where(lane >= 128 - step, ahead[gy][1 - t], ahead[gy][t])
                line.append(total + y + z)
            totals.append(line)
        return here, totals

    def sweep_one(x, _):
        here, totals = sides(start, x, 16, 2)
        for gy in range(4):
            for t in range(2):
                value = (4.0 / 3.0) * here[gy][t] + scale[t][x, gy] * totals[gy][t]
                level[t][x, gy] = value

    loop(16, T_SWEEP, sweep_one)

    def residue(pair, _):
        sums = [[None, None] for _ in range(4)]
        for k in range(2):
            x = 2 * pair + k
            here, totals = sides(level, x, 16, 2)
            for gy in range(4):
                for t in range(2):
                    r = source[t][x, gy] - (
                        diagonal[t][x, gy] * here[gy][t] - 0.125 * totals[gy][t]
                    )
                    sums[gy][t] = r if k == 0 else sums[gy][t] + r
        for gy in range(4):
            for t in range(2):
                r = 0.5 * pair_sum(sums[gy][t], lane, row)
                source_two[t][pair, gy] = scale_two[t][pair, gy] * r

    loop(8, T_REST, residue)

    def sweep_two(old, write):
        def body(x, _):
            here, totals = sides(old, x, 8, 4)
            for gy in range(4):
                for t in range(2):
                    value = (
                        (1.0 / 3.0) * here[gy][t]
                        + source_two[t][x, gy]
                        + (0.03125 * scale_two[t][x, gy]) * totals[gy][t]
                    )
                    write(x, gy, t, value)

        loop(8, T_TWO, body)

    def keep(x, gy, t, value):
        two[t][x, gy] = value

    def correct(pair, gy, t, value):
        for x in (2 * pair, 2 * pair + 1):
            level[t][x, gy] = level[t][x, gy] + value

    sweep_two(source_two, keep)
    sweep_two(two, correct)

    def last(x, _):
        here, totals = sides(level, x, 16, 2, only=1)
        gx, big = x >> 2, x & 3
        for gy in range(4):
            value = (1.0 / 3.0) * here[gy][0] + start_0[x, gy] + scale_0[x, gy] * totals[gy][0]
            out[gx * 4 + gy, pl.ds(pl.multiple_of(big * 8, 8), 8), :] = value

    loop(16, T_LAST, last)


def finish(second, got, out_hbm, out, sems):
    lane, row = lanes(), rows()
    even_lane, even_row = (lane & 1) == 0, (row & 1) == 0

    def group(g, _):
        for big in range(4):
            v = got[g, plane(big), :]
            pair = (
                jnp.where(even_lane, v, lroll(v, 1)),
                jnp.where(even_lane, lroll(v, 127), v),
            )
            for k in range(4):
                w = pair[k % 2]
                if k < 2:
                    w = jnp.where(even_row, w, sroll(w, 1))
                else:
                    w = jnp.where(even_row, sroll(w, 7), w)
                b = g * 4 + k
                for x in (2 * big, 2 * big + 1):
                    out[b, plane(x), :] = second[b, plane(x), :] + w
        return 0

    copies = []
    each = GROUPS // CHUNKS
    for i in range(CHUNKS):
        for g in range(i * each, (i + 1) * each):
            group(g, 0)
        part = pl.ds(i * (BANDS // CHUNKS), BANDS // CHUNKS)
        copies.append(pltpu.make_async_copy(out.at[part], out_hbm.at[part], sems.at[i]))
        copies[i].start()
    for copy in copies:
        copy.wait()


def swap(high, low, axis):
    size = lax.axis_size(axis)
    up = [(i, (i + 1) % size) for i in range(size)]
    return lax.ppermute(high, axis, up), lax.ppermute(low, axis, [(b, a) for a, b in up])


def in_hbm(array):
    return pltpu.with_memory_space_constraint(array, pltpu.HBM)


def local(orbitals, potential, centre, half_width):
    orb = orbitals.reshape(BANDS, 64, 128)
    pot = potential.reshape(64, 128)
    inverse = 1.0 / half_width
    face = shape(BANDS, 8, 128)
    thin, block = shape(9, 8, 128), shape(BANDS, 64, 128)

    xhi, xlo, pot = call(
        pack_x,
        [HBM] * 2,
        (face, face, shape(64, 128)),
        scratch=(pltpu.SemaphoreType.DMA((3,)),),
    )(in_hbm(orb), in_hbm(pot))
    yhi, ylo, zhi, zlo = call(pack_yz, [VMEM] * 2, (face, face, thin, thin))(orb, pot)
    zm, zp = swap(zhi, zlo, "gz")
    ym, yp = swap(yhi, ylo, "gy")
    xm, xp = swap(xhi, xlo, "gx")
    part, by_lane = call(
        first_inside, [SMEM] * 2 + [VMEM] * 2, (block, shape(2, 8, 128)), flops=BUSY
    )(centre, inverse, orb, pot)
    near = (pltpu.VMEM((64, 128), jnp.float32),)
    halos = (inverse, part, xm, xp, ym, yp, zm, zp)
    small = shape(GROUPS + 1, 8, 128)
    *faces, cxhi, cxlo, cyhi, cylo = call(
        first_faces, [SMEM] + [VMEM] * 7, (face,) * 4 + (small,) * 4, scratch=near
    )(*halos)
    cxm, cxp = swap(cxhi, cxlo, "gx")
    cym, cyp = swap(cyhi, cylo, "gy")
    (first,) = call(first_edges, [SMEM] + [VMEM] * 7, (block,), scratch=near, flops=BUSY)(*halos)
    buffer = (pltpu.VMEM((BANDS, 64, 128), jnp.float32), pltpu.SemaphoreType.DMA((CHUNKS,)))
    part, packed = call(
        second_inside,
        [SMEM] * 2 + [VMEM] * 3,
        (shape(4 * BANDS, 64, 128), shape(GROUPS, 40, 128)),
        out_specs=(HBM, VMEM),
        scratch=buffer,
        flops=BUSY,
        limit=48,
    )(centre, inverse, orb, pot, first)
    coarse, edge, xhi, xlo, yhi, ylo = call(
        coarse_edges,
        [SMEM] + [VMEM] * 11 + [ANY] * 4,
        (shape(GROUPS, 40, 128), shape(64, 128)) + (face,) * 4,
        out_specs=(HBM, VMEM) + (ANY,) * 4,
        scratch=(pltpu.VMEM((GROUPS, 40, 128), jnp.float32), pltpu.SemaphoreType.DMA((2,))),
        aliases={12: 2, 13: 3, 14: 4, 15: 5},
    )(inverse, by_lane, pot, packed, cxm, cxp, cym, cyp, zm, zp, zhi, zlo, *faces)
    got = lax.all_to_all(coarse, ("gx", "gy"), 0, 0, tiled=True)
    xm, xp = swap(xhi, xlo, "gx")
    ym, yp = swap(yhi, ylo, "gy")
    (second,) = call(
        second_edges, [SMEM, HBM] + [VMEM] * 5, (block,), scratch=buffer, flops=BUSY, limit=48
    )(inverse, part, xm, xp, ym, yp, edge)
    ends = shape(10, 8, 128)
    mhi, mlo = call(pack_ends, [VMEM], (ends, ends))(got)
    left, right = swap(mhi, mlo, "gz")
    lines, half = (16, 4, 8, 128), (8, 4, 8, 128)
    terms = call(
        open_block, [VMEM], (shape(*lines),) * 4 + (shape(*half),), flops=BUSY
    )(got)
    lines, half = pltpu.VMEM(lines, jnp.float32), pltpu.VMEM(half, jnp.float32)
    (level,) = call(
        coarse_solve,
        [VMEM] * 8,
        (shape(GROUPS, 32, 128),),
        scratch=(lines,) * 4 + (half,) + (lines,) * 2 + (half,) * 4,
        limit=6,
    )(left, right, *terms, second)
    level = lax.all_to_all(level, ("gx", "gy"), 0, 0, tiled=True)
    (out,) = call(
        finish,
        [VMEM] * 2,
        (block,),
        out_specs=(HBM,),
        scratch=(pltpu.VMEM((BANDS, 64, 128), jnp.float32), pltpu.SemaphoreType.DMA((CHUNKS,))),
        limit=4,
    )(second, level)
    return out.reshape(BANDS, 8, 8, 128)


def solution(mesh):
    in_specs = (P(None, "gx", "gy", "gz"), P("gx", "gy", "gz"), P(), P())
    out_specs = P(None, "gx", "gy", "gz")
    return jax.shard_map(local, mesh=mesh, in_specs=in_specs, out_specs=out_specs, check_vma=False)
```
